256 devices in a mesh: row: 16 (over x, z_lo, core), col: 16 (over z_hi, y).
Axes of the slice: x: 4, y: 4, z: 8 (z_hi: 4, z_lo: 2; z = z_hi * 2 + z_lo), core: 2. Of those that a mesh axis runs over, the one named last changes fastest.
Arguments:
- first_set: float32 [16384, 128], P(('row', 'col')), may hold values from -64 to 64, as said below
- second_set: float32 [16384, 128], P(('row', 'col')), may hold values from -64 to 64, as said below
- query_weight: float32 [2, 128, 128], replicated, may hold values from -0.5 to 0.5
- key_weight: float32 [2, 128, 128], replicated, may hold values from -0.5 to 0.5
- norm_gain: float32 [2, 128], replicated, may hold values from 0.25 to 1.75
- up_weight: float32 [2, 128, 512], replicated, may hold values from -0.5 to 0.5
- up_bias: float32 [2, 512], replicated, may hold values from -3 to 3
- down_weight: float32 [2, 512, 128], replicated, may hold values from -0.25 to 0.25
Outputs:
- first_out: float32 [16384, 128], P(('row', 'col'))
- second_out: float32 [16384, 128], P(('row', 'col'))
The draws below stay inside these ranges and needn't reach their ends.
Inputs may be any that keep to these rules, and one draw needn't show every extreme that they name: `first_set`: rows have differing scales. `second_set`: rows have differing scales.
All inputs are finite; a program needn't handle non-finite values.
Results may differ from the reference program's by a relative error of at most 0.0004.
Values sent between devices are 32-bit elements; how exact they have to be, the bound alone decides.
A program may use at most 64 MiB of HBM per device.

```python
import math
import jax
import jax.numpy as jnp
from jax import lax

D = 128
HID = 512
LAYERS = 2
NA = 16384
NB = 16384


def draw_features(key, count):
    key_base = jax.random.fold_in(key, 11)
    key_scale = jax.random.fold_in(key, 12)
    base = jnp.clip(jax.random.normal(key_base, (count, D), jnp.float32), -6.0, 6.0)
    scales = jnp.exp(jax.random.uniform(key_scale, (count,), jnp.float32, jnp.log(0.5), jnp.log(2.0)))
    return base * scales[:, None]


def draw_first_set(key, part):
    return draw_features(jax.random.fold_in(key, 1), NA)


def draw_second_set(key, part):
    return draw_features(jax.random.fold_in(key, 2), NB)


def scatter_about(key, extent, deviation, reach, kind=jnp.bfloat16):
    drawn = jax.random.normal(key, extent, jnp.float32) * deviation
    return jnp.minimum(jnp.maximum(drawn, -reach), reach).astype(kind)


def setup_inputs(seed: int = 0) -> dict:
    arg_keys = jax.random.split(jax.random.key(seed), 9)
    return {
        "first_set": draw_first_set(jax.random.fold_in(arg_keys[8], 71), 0),
        "second_set": draw_second_set(jax.random.fold_in(arg_keys[8], 71), 0),
        "query_weight": scatter_about(arg_keys[2], (LAYERS, D, D), D ** -0.5, 0.5, jnp.float32),
        "key_weight": scatter_about(arg_keys[3], (LAYERS, D, D), D ** -0.5, 0.5, jnp.float32),
        "norm_gain": jnp.clip(1.0 + 0.15 * jax.random.normal(arg_keys[4], (LAYERS, D), jnp.float32), 0.25, 1.75),
        "up_weight": scatter_about(arg_keys[5], (LAYERS, D, HID), D ** -0.5, 0.5, jnp.float32),
        "up_bias": scatter_about(arg_keys[6], (LAYERS, HID), 0.5, 3.0, jnp.float32),
        "down_weight": scatter_about(arg_keys[7], (LAYERS, HID, D), HID ** -0.5, 0.25, jnp.float32),
    }


HIGH = lax.Precision.HIGHEST

def refine(hidden, gain, w_up, b_up, w_down):
    scale = lax.rsqrt(lax.optimization_barrier(jnp.mean(hidden * hidden, axis=1, keepdims=True)) + 1e-05)
    normed = hidden * scale * gain
    inner = jax.nn.gelu(jnp.dot(normed, w_up, precision=HIGH) + b_up)
    return hidden + jnp.dot(inner, w_down, precision=HIGH)

def align(first, second, w_query, w_key, gain, w_up, b_up, w_down):
    width = first.shape[1]
    factor = 2.0 / math.sqrt(width)
    block = math.gcd(NA, 1024)
    count = NA // block
    queries = jnp.dot(first, w_query, precision=HIGH).reshape(count, block, width)
    keyed = jnp.dot(second, w_key, precision=HIGH)
    first_blocks = first.reshape(count, block, width)

    def scores_of(query_blk):
        return jnp.dot(query_blk, keyed.T, precision=HIGH) * factor

    def pass_max(carry, query_blk):
        tile = scores_of(query_blk)
        return (jnp.maximum(carry, lax.optimization_barrier(jnp.max(tile, axis=0))), lax.optimization_barrier(jnp.max(tile, axis=1)))
    col_max, row_max = lax.scan(pass_max, jnp.full((NB,), -jnp.inf, jnp.float32), queries)

    def pass_sum(carry, inputs):
        query_blk, peak = inputs
        tile = scores_of(query_blk)
        col_part = lax.optimization_barrier(jnp.sum(jnp.exp(tile - col_max[None, :]), axis=0))
        return (carry + col_part, lax.optimization_barrier(jnp.sum(jnp.exp(tile - peak[:, None]), axis=1)))
    col_sum, row_sum = lax.scan(pass_sum, jnp.zeros((NB,), jnp.float32), (queries, row_max))

    def pass_message(carry, inputs):
        query_blk, peak, total, rows_blk = inputs
        message_acc, mass_acc = carry
        tile = scores_of(query_blk)
        match = jnp.exp(tile - peak[:, None]) / total[:, None] * (jnp.exp(tile - col_max[None, :]) / col_sum[None, :])
        to_first = jnp.dot(match, second, precision=HIGH)
        row_mass = lax.optimization_barrier(jnp.sum(match, axis=1))
        new_carry = (message_acc + jnp.dot(match.T, rows_blk, precision=HIGH), mass_acc + lax.optimization_barrier(jnp.sum(match, axis=0)))
        return (new_carry, (to_first, row_mass))
    start = (jnp.zeros((NB, width), jnp.float32), jnp.zeros((NB,), jnp.float32))
    (to_second, col_mass), (to_first, row_mass) = lax.scan(pass_message, start, (queries, row_max, row_sum, first_blocks))
    to_first = to_first.reshape(NA, width) / (row_mass.reshape(NA) + 0.05 / NB)[:, None]
    to_second = to_second / (col_mass + 0.05 / NA)[:, None]
    hx = first + to_first
    hy = second + to_second
    return (refine(hx, gain, w_up, b_up, w_down), refine(hy, gain, w_up, b_up, w_down))

def reference(first_set, second_set, query_weight, key_weight, norm_gain, up_weight, up_bias, down_weight):
    first, second = (first_set, second_set)
    for layer_idx in range(LAYERS):
        first, second = align(first, second, query_weight[layer_idx], key_weight[layer_idx], norm_gain[layer_idx], up_weight[layer_idx], up_bias[layer_idx], down_weight[layer_idx])
    return (first, second)
```

```python
import functools
import math

import jax
import jax.numpy as jnp
from jax import lax
from jax.experimental import pallas as pl
from jax.experimental.pallas import tpu as pltpu
from jax.sharding import PartitionSpec as P

MESH = pl.DeviceIdType.MESH
F32, BF16 = jnp.float32, jnp.bfloat16
HIGH = lax.Precision.HIGHEST
LOG2E = math.log2(math.e)
NT = (((1,), (1,)), ((), ()))


def dot(a, b, dims=(((1,), (0,)), ((), ()))):
    return lax.dot_general(a, b, dims, preferred_element_type=F32)


def high(a, b, dims=(((1,), (0,)), ((), ()))):
    return lax.dot_general(a, b, dims, precision=HIGH, preferred_element_type=F32)


def split2(v):
    top = v.astype(BF16)
    return top, (v - top.astype(F32)).astype(BF16)


def split3(v):
    top = v.astype(BF16)
    rest = v - top.astype(F32)
    mid = rest.astype(BF16)
    return top, mid, (rest - mid.astype(F32)).astype(BF16)


def eye(rows, shift=0):
    r = lax.broadcasted_iota(jnp.int32, (rows, 128), 0)
    c = lax.broadcasted_iota(jnp.int32, (rows, 128), 1)
    return c == r + shift


def to_lanes(column, mask):
    spread = jnp.broadcast_to(column, mask.shape)
    return jnp.sum(jnp.where(mask, spread, 0.0), axis=0, keepdims=True)


def to_rows(line, mask):
    spread = jnp.broadcast_to(line, mask.shape)
    return jnp.sum(jnp.where(mask, spread, 0.0), axis=1, keepdims=True)


def kernel(
    dims, total, x_ref, y_ref, wq, wk, gain, up, bias, down, o1, o2,
    A, B, S, MH, ML, T1, T2, K1, K2, K3, AT, BC, RM, RS, RB, RW,
    rsend, csend, rgot, cgot, PS, PR, QS, QX, QR,
    sa, ra_, sb, rb_, sf, rf, ssr, rsr, ssc, rsc, sp, rp, sx, rx, sq, rq,
):
    nx, ny, nz = dims
    ga, gb = nx * ny, nz * 2
    row, col = lax.axis_index("row"), lax.axis_index("col")
    x, zl, k = lax.div(row, 4), lax.rem(lax.div(row, 2), 2), lax.rem(row, 2)
    zh, y = lax.div(col, ny), lax.rem(col, ny)
    z = zh * 2 + zl
    me_a, me_b = x * ny + y, z * 2 + k
    blk = x_ref.shape[0]
    rows, cols = ga * blk, gb * blk
    rchunk, cchunk = min(256, rows), min(256, cols)
    offset = 0.05 / total
    factor = 2.0 / math.sqrt(x_ref.shape[1]) * LOG2E
    pad = PS.shape[1]

    def at(x, y, z, k):
        return (x * 4 + lax.rem(z, 2) * 2 + k, lax.div(z, 2) * ny + y)

    def plane(n):
        dx, dy = n
        px, py = lax.rem(x + dx, nx), lax.rem(y + dy, ny)
        return px * ny + py, at(px, py, z, k)

    def line(dz, other):
        pz = lax.rem(z + dz, nz)
        pk = 1 - k if other else k
        return pz * 2 + pk, at(x, y, pz, pk)

    near = lambda d, n: min(d, n - d)
    plane_steps = sorted(
        [(dx, dy) for dx in range(nx) for dy in range(ny) if (dx, dy) != (0, 0)],
        key=lambda s: -near(s[0], nx) - near(s[1], ny),
    )
    z_steps = sorted(range(1, nz), key=lambda d: near(d, nz))
    line_steps = [(d, o) for d in [*z_steps[::-1], 0] for o in (False, True) if (d, o) != (0, False)]

    def copy(src, dst, ss, rs, dev):
        return pltpu.make_async_remote_copy(
            src_ref=src, dst_ref=dst, send_sem=ss, recv_sem=rs, device_id=dev, device_id_type=MESH
        )

    barrier = pltpu.get_barrier_semaphore()
    for step in plane_steps:
        pl.semaphore_signal(barrier, inc=1, device_id=plane(step)[1], device_id_type=MESH)
    for step in line_steps:
        pl.semaphore_signal(barrier, inc=1, device_id=line(*step)[1], device_id_type=MESH)
    o1[...] = x_ref[...]
    o2[...] = y_ref[...]
    pl.semaphore_wait(barrier, len(plane_steps) + len(line_steps))

    def slot(n):
        return pl.ds(pl.multiple_of(n * blk, blk), blk)

    def layer(l, carry):
        A[l, slot(me_a), :] = o1[...]
        B[l, slot(me_b), :] = o2[...]
        sent = []

        def send(src, dst, ss, rs, dev):
            c = copy(src, dst, ss, rs, dev)
            c.start()
            sent.append(c)

        own_a, own_b = A.at[l, slot(me_a)], B.at[l, slot(me_b)]
        _, sibling = line(0, True)
        send(own_b, own_b, sb.at[l, nz - 1], rf.at[l, z], sibling)
        for n, d in enumerate(z_steps[::-1]):
            send(own_b, own_b, sb.at[l, n], rb_.at[l, z], line(d, False)[1])
        for n, step in enumerate(plane_steps):
            send(own_a, own_a, sa.at[l, n], ra_.at[l, me_a], plane(step)[1])

        mix = high(wk[l], wq[l], NT) * factor

        for n, d in enumerate(z_steps):
            s, dev = line(d, False)
            ref = B.at[l, slot(s)]
            pz = lax.rem(z + d, nz)
            copy(ref, ref, sf.at[l, n], rb_.at[l, pz], sibling).wait_recv()
            send(ref, ref, sf.at[l, n], rf.at[l, pz], sibling)
        for d in range(nz):
            s, dev = line(d, True)
            ref = B.at[l, slot(s)]
            copy(ref, ref, sf.at[l, 0], rf.at[l, lax.rem(z + d, nz)], sibling).wait_recv()

        def make_keys(n, c):
            at_ = pl.ds(pl.multiple_of(n * 128, 128), 128)
            v = B[l, at_, :]
            b1, b2 = split2(v)
            BC[at_, 0:128] = b1
            BC[at_, 128:256] = b2
            k1, k2, k3 = split3(high(v, mix))
            K1[at_, 0:128] = k1
            K1[at_, 128:256] = k2
            K2[at_, 0:128] = k2
            K2[at_, 128:256] = k1
            K3[at_, 0:128] = k3
            K3[at_, 128:256] = k1
            return c

        lax.fori_loop(0, cols // 128, make_keys, 0)

        for step in plane_steps[::-1]:
            s, dev = plane(step)
            ref = A.at[l, slot(s)]
            copy(ref, ref, sa.at[l, 0], ra_.at[l, s], dev).wait_recv()

        def make_rows(n, c):
            at_ = pl.ds(pl.multiple_of(n * 128, 128), 128)
            v = A[l, at_, :]
            a1, a2, a3 = split3(v)
            T1[at_, 0:128] = a1
            T1[at_, 128:256] = a2
            T2[at_, 0:128] = a1
            T2[at_, 128:256] = a3
            t1, t2 = split2(v.T)
            AT[0:128, at_] = t1
            AT[128:256, at_] = t2
            return c

        lax.fori_loop(0, rows // 128, make_rows, 0)

        def score(n, carry):
            cm, cs = carry
            at_ = pl.ds(pl.multiple_of(n * rchunk, rchunk), rchunk)
            t1, t2 = T1[at_, :], T2[at_, :]
            S[at_, :] = dot(t1, K1[...], NT) + dot(t1, K2[...], NT) + dot(t2, K3[...], NT)
            base = n * rchunk

            def peak(i, m):
                for u in range(4):
                    m = jnp.maximum(m, S[pl.ds(pl.multiple_of(base + i * 32 + u * 8, 8), 8), :])
                return m

            new = lax.fori_loop(0, rchunk // 32, peak, cm)
            cs = cs * jnp.exp2(cm - new)

            def sums(i, c):
                for u in range(4):
                    r = pl.ds(pl.multiple_of(base + i * 32 + u * 8, 8), 8)
                    s = S[r, :]
                    parts = [s[:, j * 128 : (j + 1) * 128] for j in range(cols // 128)]
                    m = functools.reduce(jnp.maximum, parts)
                    RM[r, :] = m
                    RS[r, :] = functools.reduce(jnp.add, [jnp.exp2(p - m) for p in parts])
                    c = c + jnp.exp2(s - new)
                return c

            return new, lax.fori_loop(0, rchunk // 32, sums, cs)

        cm, cs = lax.fori_loop(
            0, rows // rchunk, score,
            (jnp.full((8, cols), -jnp.inf, F32), jnp.zeros((8, cols), F32)),
        )
        cpeak = jnp.max(cm, axis=0, keepdims=True)
        clse = cpeak + jnp.log(jnp.sum(cs * jnp.exp2(cm - cpeak), axis=0, keepdims=True)) * LOG2E
        for j in range(cols // 128):
            csend[j : j + 1, :] = clse[:, j * 128 : (j + 1) * 128]
        same = eye(128)

        def row_lse(n, c):
            at_ = pl.ds(pl.multiple_of(n * 128, 128), 128)
            m = RM[at_, :]
            p = jnp.max(m, axis=1, keepdims=True)
            t = jnp.sum(RS[at_, :] * jnp.exp2(m - p), axis=1, keepdims=True)
            rsend[pl.ds(n, 1), :] = to_lanes(p + jnp.log(t) * LOG2E, same)
            return c

        for n, step in enumerate(line_steps):
            send(csend, cgot.at[l, me_b], ssc.at[l, n], rsc.at[l, me_b], line(*step)[1])
        lax.fori_loop(0, rows // 128, row_lse, 0)

        for n, step in enumerate(plane_steps):
            send(rsend, rgot.at[l, me_a], ssr.at[l, n], rsr.at[l, me_a], plane(step)[1])
        cgot[l, me_b] = csend[...]
        rgot[l, me_a] = rsend[...]
        for step in plane_steps[::-1]:
            s, dev = plane(step)
            copy(rsend, rgot.at[l, s], ssr.at[l, 0], rsr.at[l, s], dev).wait_recv()

        def lse(got):
            p = jnp.max(got, axis=0)
            return p + jnp.log(jnp.sum(jnp.exp2(got - p), axis=0)) * LOG2E

        rw = lse(rgot[l])
        RW[...] = rw

        def spread(n, c):
            at_ = pl.ds(pl.multiple_of(n * 128, 128), 128)
            RB[at_, :] = jnp.broadcast_to(to_rows(RW[pl.ds(n, 1), :], same), (128, 128))
            RM[at_, :] = jnp.zeros((128, 128), F32)
            return c

        lax.fori_loop(0, rows // 128, spread, 0)
        for step in line_steps[::-1]:
            s, dev = line(*step)
            copy(csend, cgot.at[l, s], ssc.at[l, 0], rsc.at[l, s], dev).wait_recv()
        RW[...] = lse(cgot[l])

        lanes = cchunk // 128
        per = cchunk // blk

        def columns(n, carry):
            at_ = pl.ds(pl.multiple_of(n * cchunk, cchunk), cchunk)
            c = jnp.concatenate([RW[pl.ds(n * lanes + j, 1), :] for j in range(lanes)], axis=1)
            cb = jnp.broadcast_to(c, (16, cchunk))

            def piece(i, mass):
                for u in range(4):
                    r = pl.ds(pl.multiple_of(i * 64 + u * 16, 16), 16)
                    s = S[r, at_]
                    rb = RB[r, :]
                    rb = jnp.concatenate([rb] * lanes, axis=1)
                    m = jnp.exp2((s - rb) + (s - cb))
                    RM[r, :] += functools.reduce(
                        jnp.add, [m[:, j * 128 : (j + 1) * 128] for j in range(lanes)]
                    )
                    mass = mass + (m[0:8] + m[8:16])
                    h, lo = split2(m)
                    MH[r, at_] = h
                    ML[r, at_] = lo
                return mass

            mass = lax.fori_loop(0, rows // 64, piece, jnp.zeros((8, cchunk), F32))
            mass = jnp.sum(mass, axis=0, keepdims=True)
            q = dot(AT[...], MH[:, at_])
            q = q[0:128] + q[128:256] + dot(AT[0:128, :], ML[:, at_])
            for j in range(lanes):
                t = q[:, j * 128 : (j + 1) * 128].T
                for b in range(128 // blk):
                    QS[n * per + j * (128 // blk) + b, 0:blk, :] = t[b * blk : (b + 1) * blk]
                    QS[n * per + j * (128 // blk) + b, blk:pad, :] = jnp.broadcast_to(
                        mass[:, j * 128 : (j + 1) * 128], (pad - blk, 128)
                    )
            for b in range(per // 2):
                zz = n * (per // 2) + b
                copy(
                    QS.at[zz * 2 + (1 - k)], QX.at[l, zz], sx.at[l, zz], rx.at[l, zz], sibling
                ).start()
            return carry

        lax.fori_loop(0, cols // cchunk, columns, 0)

        small = eye(blk)

        def messages(n, carry):
            at_ = pl.ds(pl.multiple_of(n * rchunk, rchunk), rchunk)
            p = dot(MH[at_, :], BC[...])
            p = p[:, 0:128] + p[:, 128:256] + dot(ML[at_, :], BC[:, 0:128])
            mass = jnp.sum(RM[at_, :], axis=1, keepdims=True)
            for b in range(rchunk // blk):
                PS[n * (rchunk // blk) + b, 0:blk, :] = p[b * blk : (b + 1) * blk]
                PS[n * (rchunk // blk) + b, blk:pad, :] = jnp.broadcast_to(
                    to_lanes(mass[b * blk : (b + 1) * blk], small), (pad - blk, 128)
                )
            return carry

        def forward(zz):
            copy(
                QS.at[zz * 2 + (1 - k)], QX.at[l, zz], sx.at[l, zz], rx.at[l, zz], sibling
            ).wait_recv()
            return QS[zz * 2 + k] + QX[l, zz]

        for n, d in enumerate(z_steps[::-1]):
            pz = lax.rem(z + d, nz)
            QS[pz * 2 + k] = forward(pz)
            send(QS.at[pz * 2 + k], QR.at[l, z], sq.at[l, n], rq.at[l, z], line(d, False)[1])
        QR[l, z] = forward(z)

        lax.fori_loop(0, rows // rchunk, messages, 0)
        for n, step in enumerate(plane_steps):
            s, dev = plane(step)
            send(PS.at[s], PR.at[l, me_a], sp.at[l, n], rp.at[l, me_a], dev)
        PR[l, me_a] = PS[me_a]

        for n, d in enumerate(z_steps):
            s, dev = line(d, False)
            pz = lax.rem(z + d, nz)
            copy(QS.at[0], QR.at[l, pz], sq.at[l, 0], rq.at[l, pz], dev).wait_recv()
        q = jnp.sum(QR[l], axis=0)
        for step in plane_steps[::-1]:
            s, dev = plane(step)
            copy(PS.at[0], PR.at[l, s], sp.at[l, 0], rp.at[l, s], dev).wait_recv()
        p = jnp.sum(PR[l], axis=0)
        pm = to_rows(p[blk : blk + 1], small)
        qm = to_rows(q[blk : blk + 1], eye(blk, lax.rem(me_b, 128 // blk) * blk))
        hx = o1[...] + p[0:blk] / (pm + offset)
        hy = o2[...] + q[0:blk] / (qm + offset)
        h = jnp.concatenate([hx, hy], axis=0)
        scale = lax.rsqrt(jnp.mean(h * h, axis=1, keepdims=True) + 1e-05)
        u = high(h * scale * gain[l], up[l]) + bias[l]
        g = 0.5 * u * (1.0 + jnp.tanh(math.sqrt(2 / math.pi) * (u + 0.044715 * (u * u * u))))
        h = h + high(g, down[l])
        o1[...] = h[0:blk]
        o2[...] = h[blk : 2 * blk]
        for c in sent:
            c.wait_send()
        for zz in range(nz):
            copy(QS.at[zz * 2 + (1 - k)], QX.at[l, zz], sx.at[l, zz], rx.at[l, zz], sibling).wait_send()
        return carry

    lax.fori_loop(0, 2, layer, 0)


def align_all(dims, x, y, wq, wk, gain, up, bias, down):
    nx, ny, nz = dims
    ga, gb = nx * ny, nz * 2
    blk, d = x.shape
    rows, cols = ga * blk, gb * blk
    L = wq.shape[0]
    pad = blk + 8
    V, dma = pltpu.VMEM, lambda *s: pltpu.SemaphoreType.DMA(s)
    body = functools.partial(kernel, dims, blk * ga * gb)
    return pl.pallas_call(
        body,
        out_shape=[jax.ShapeDtypeStruct((blk, d), F32)] * 2,
        in_specs=[pl.BlockSpec(memory_space=V)] * 8,
        out_specs=[pl.BlockSpec(memory_space=V)] * 2,
        scratch_shapes=[
            V((L, rows, d), F32), V((L, cols, d), F32), V((rows, cols), F32),
            V((rows, cols), BF16), V((rows, cols), BF16),
            V((rows, 2 * d), BF16), V((rows, 2 * d), BF16),
            V((cols, 2 * d), BF16), V((cols, 2 * d), BF16), V((cols, 2 * d), BF16),
            V((2 * d, rows), BF16), V((cols, 2 * d), BF16),
            V((rows, 128), F32), V((rows, 128), F32), V((rows, 128), F32),
            V((max(rows, cols) // 128, 128), F32),
            V((rows // 128, 128), F32), V((cols // 128, 128), F32),
            V((L, ga, rows // 128, 128), F32), V((L, gb, cols // 128, 128), F32),
            V((ga, pad, d), F32), V((L, ga, pad, d), F32),
            V((gb, pad, d), F32), V((L, nz, pad, d), F32), V((L, nz, pad, d), F32),
            dma(L, ga), dma(L, ga), dma(L, nz), dma(L, nz), dma(L, nz), dma(L, nz),
            dma(L, ga), dma(L, ga), dma(L, gb), dma(L, gb),
            dma(L, ga), dma(L, ga), dma(L, nz), dma(L, nz), dma(L, nz), dma(L, nz),
        ],
        compiler_params=pltpu.CompilerParams(
            collective_id=0, has_side_effects=True, vmem_limit_bytes=60 * 1024 * 1024
        ),
    )(x, y, wq, wk, gain[:, None, :], up, bias[:, None, :], down)


def solution(mesh):
    size = mesh.shape["row"] * mesh.shape["col"]
    dims = (4, 4, 8) if size == 256 else (2, 2, 2)
    placed = (P(("row", "col"), None), P(("row", "col"), None), P(), P(), P(), P(), P(), P())
    return jax.shard_map(
        functools.partial(align_all, dims),
        mesh=mesh,
        in_specs=placed,
        out_specs=(P(("row", "col"), None), P(("row", "col"), None)),
        check_vma=False,
    )
```

```python
import functools
import math

import jax
import jax.numpy as jnp
from jax import lax
from jax.experimental import pallas as pl
from jax.experimental.pallas import tpu as pltpu
from jax.sharding import PartitionSpec as P

MESH = pl.DeviceIdType.MESH
F32, BF16 = jnp.float32, jnp.bfloat16
HIGH = lax.Precision.HIGHEST
LOG2E = math.log2(math.e)
NT = (((1,), (1,)), ((), ()))


def dot(a, b, dims=(((1,), (0,)), ((), ()))):
    return lax.dot_general(a, b, dims, preferred_element_type=F32)


def high(a, b, dims=(((1,), (0,)), ((), ()))):
    return lax.dot_general(a, b, dims, precision=HIGH, preferred_element_type=F32)


def split2(v):
    top = v.astype(BF16)
    return top, (v - top.astype(F32)).astype(BF16)


def split3(v):
    top = v.astype(BF16)
    rest = v - top.astype(F32)
    mid = rest.astype(BF16)
    return top, mid, (rest - mid.astype(F32)).astype(BF16)


def eye(rows, shift=0):
    r = lax.broadcasted_iota(jnp.int32, (rows, 128), 0)
    c = lax.broadcasted_iota(jnp.int32, (rows, 128), 1)
    return c == r + shift


def to_lanes(column, mask):
    spread = jnp.broadcast_to(column, mask.shape)
    return jnp.sum(jnp.where(mask, spread, 0.0), axis=0, keepdims=True)


def to_rows(line, mask):
    spread = jnp.broadcast_to(line, mask.shape)
    return jnp.sum(jnp.where(mask, spread, 0.0), axis=1, keepdims=True)


def kernel(
    dims, total, x_ref, y_ref, wq_h, wk_h, gain_h, up_h, bias_h, down_h, out,
    A, B, S, E, MH, ML, T1, T2, K1, K2, K3, AF, AT, BC, RM, RS, RB, RW, CW,
    rsend, csend, rgot, cgot, PS, PR, QS, QX, QR,
    wq, wk, gain, up, bias, down,
    sl, sa, ra_, sb, rb_, rf, ssr, rsr, ssc, rsc, sp, rp, sx, rx, sq, rq,
):
    nx, ny, nz = dims
    row, col = lax.axis_index("row"), lax.axis_index("col")
    x, zl, k = lax.div(row, 4), lax.rem(lax.div(row, 2), 2), lax.rem(row, 2)
    zh, y = lax.div(col, ny), lax.rem(col, ny)
    z = zh * 2 + zl
    me_a, me_b = x * ny + y, z * 2 + k
    blk = x_ref.shape[0]
    rows, cols = nx * ny * blk, nz * 2 * blk
    rchunk, cchunk, schunk = ny * blk, 256, min(512, rows)
    lanes = cchunk // 128
    offset = 0.05 / total
    factor = 2.0 / math.sqrt(x_ref.shape[1]) * LOG2E
    pad = PS.shape[1]
    scope = jax.named_scope

    def at(x, y, z, k):
        return (x * 4 + lax.rem(z, 2) * 2 + k, lax.div(z, 2) * ny + y)

    def plane(n):
        px, py = lax.rem(x + n[0], nx), lax.rem(y + n[1], ny)
        return px * ny + py, at(px, py, z, k)

    def line(dz, other):
        pz = lax.rem(z + dz, nz)
        pk = 1 - k if other else k
        return pz * 2 + pk, at(x, y, pz, pk)

    near = lambda d, n: min(d, n - d)
    plane_steps = sorted(
        [(dx, dy) for dx in range(nx) for dy in range(ny) if (dx, dy) != (0, 0)],
        key=lambda s: -near(s[0], nx) - near(s[1], ny),
    )
    z_steps = sorted(range(1, nz), key=lambda d: near(d, nz))
    line_steps = [(d, o) for d in [*z_steps[::-1], 0] for o in (False, True) if (d, o) != (0, False)]
    _, sibling = line(0, True)

    def copy(src, dst, ss, rs, dev):
        return pltpu.make_async_remote_copy(
            src_ref=src, dst_ref=dst, send_sem=ss, recv_sem=rs, device_id=dev, device_id_type=MESH
        )

    def slot(n):
        return pl.ds(pl.multiple_of(n * blk, blk), blk)

    def chunk(n, size):
        return pl.ds(pl.multiple_of(n * size, size), size)

    with scope("entry"):
        barrier = pltpu.get_barrier_semaphore()
        for step in plane_steps:
            pl.semaphore_signal(barrier, inc=1, device_id=plane(step)[1], device_id_type=MESH)
        for step in line_steps:
            pl.semaphore_signal(barrier, inc=1, device_id=line(*step)[1], device_id_type=MESH)
        moves = [
            (x_ref, A.at[0, slot(me_a)]), (y_ref, B.at[0, slot(me_b)]), (wq_h, wq), (wk_h, wk),
            (gain_h, gain), (up_h, up), (bias_h, bias), (down_h, down),
        ]
        moves = [pltpu.make_async_copy(a, b, sl.at[n]) for n, (a, b) in enumerate(moves)]
        for m in moves:
            m.start()
        for m in moves[:2]:
            m.wait()
        pl.semaphore_wait(barrier, len(plane_steps) + len(line_steps))

    same, small = eye(128), eye(blk)

    def layer(l, carry):
        def send(src, dst, ss, rs, dev):
            copy(src, dst, ss.at[l], rs, dev).start()

        def whole(ref, ss, rs):
            return copy(ref, ref, ss.at[l], rs, sibling)

        own_a, own_b = A.at[l, slot(me_a)], B.at[l, slot(me_b)]
        send(own_b, own_b, sb, rf.at[l], sibling)
        for n, d in enumerate(z_steps[::-1]):
            send(own_b, own_b, sb, rb_.at[l, z], line(d, False)[1])
        for n, step in enumerate(plane_steps):
            send(own_a, own_a, sa, ra_.at[l], plane(step)[1])

        @pl.when(l == 0)
        def _():
            for m in moves[2:]:
                m.wait()

        mix = high(wk[l], wq[l], NT) * factor

        def make_keys(at_):
            k1, k2, k3 = split3(high(B[l, at_, :], mix))
            K1[at_, 0:128] = k1
            K1[at_, 128:256] = k2
            K2[at_, 0:128] = k2
            K2[at_, 128:256] = k1
            K3[at_, 0:128] = k3
            K3[at_, 128:256] = k1

        def make_rows(at_):
            a1, a2, a3 = split3(A[l, at_, :])
            T1[at_, 0:128] = a1
            T1[at_, 128:256] = a2
            T2[at_, 0:128] = a1
            T2[at_, 128:256] = a3

        with scope("gather"):
            for d in z_steps[::-1]:
                s, _ = line(d, False)
                ref, pz = B.at[l, slot(s)], lax.rem(z + d, nz)
                whole(ref, sb, rb_.at[l, pz]).wait_recv()
                send(ref, ref, sb, rf.at[l], sibling)
            whole(A.at[l, pl.ds(0, rows - blk)], sa, ra_.at[l]).wait_recv()
            whole(B.at[l, pl.ds(0, cols // 2)], sb, rf.at[l]).wait_recv()
        with scope("operands"):
            for n in range(cols // 256):
                make_keys(pl.ds(n * 256, 256))
            for n in range(rows // 256):
                make_rows(pl.ds(n * 256, 256))

        def product(n):
            at_ = pl.ds(n * schunk, schunk)
            t1, t2 = T1[at_, :], T2[at_, :]
            S[at_, :] = dot(t1, K1[...], NT) + dot(t1, K2[...], NT) + dot(t2, K3[...], NT)

        def statistics(n, cm, cs):
            base = n * schunk
            new = cm
            for i in range(0, schunk, 8):
                new = jnp.maximum(new, S[base + i : base + i + 8, :])
            cs = cs * jnp.exp2(cm - new)
            for i in range(0, schunk, 8):
                r = pl.ds(base + i, 8)
                s = S[r, :]
                parts = [s[:, j * 128 : (j + 1) * 128] for j in range(cols // 128)]
                m = functools.reduce(jnp.maximum, parts)
                RM[r, :] = m
                RS[r, :] = functools.reduce(jnp.add, [jnp.exp2(p - m) for p in parts])
                cs = cs + jnp.exp2(s - new)
            return new, cs

        def row_lse(n):
            at_ = pl.ds(n * 128, 128)
            m = RM[at_, :]
            p = jnp.max(m, axis=1, keepdims=True)
            t = jnp.sum(RS[at_, :] * jnp.exp2(m - p), axis=1, keepdims=True)
            own = jnp.broadcast_to(p + jnp.log(t) * LOG2E, (128, 128))
            RB[at_, :] = own
            rsend[n : n + 1, :] = to_lanes(own, same)

        with scope("score"):
            cm, cs = jnp.full((8, cols), -jnp.inf, F32), jnp.zeros((8, cols), F32)
            product(0)
            for n in range(rows // schunk):
                if n + 1 < rows // schunk:
                    product(n + 1)
                cm, cs = statistics(n, cm, cs)
        with scope("lse"):
            cpeak = jnp.max(cm, axis=0, keepdims=True)
            clse = cpeak + jnp.log(jnp.sum(cs * jnp.exp2(cm - cpeak), axis=0, keepdims=True)) * LOG2E
            for j in range(cols // 128):
                csend[j : j + 1, :] = clse[:, j * 128 : (j + 1) * 128]
            for n, step in enumerate(line_steps):
                send(csend, cgot.at[l, me_b], ssc, rsc.at[l], line(*step)[1])
            for n in range(rows // 128):
                row_lse(n)
            for n, step in enumerate(plane_steps):
                send(rsend, rgot.at[l, me_a], ssr, rsr.at[l], plane(step)[1])
        cgot[l, me_b] = csend[...]
        rgot[l, me_a] = rsend[...]
        turns = {4: (2, 1, 3, 0), 2: (1, 0), 1: (0,)}
        cturn, rturn = turns[cols // cchunk], turns[rows // rchunk]

        def column_line(ref, b):
            return jnp.concatenate([ref[pl.ds(b * lanes + j, 1), :] for j in range(lanes)], axis=1)

        def matches(n):
            b = lax.rem(zh + cturn[n], len(cturn))
            at_ = chunk(b, cchunk)
            cb = jnp.broadcast_to(column_line(csend, b), (16, cchunk))
            for i in range(0, rows, 16):
                r = pl.ds(i, 16)
                s = S[r, at_]
                rb = RB[r, :]
                m = jnp.exp2((s - jnp.concatenate([rb] * lanes, axis=1)) + (s - cb))
                E[n, r, :] = m
                h, lo = split2(m)
                MH[n, r, :] = h
                ML[n, r, :] = lo

        with scope("match"):
            for n in range(rows // 128):
                AF[:, n * 128 : (n + 1) * 128] = A[l, n * 128 : (n + 1) * 128, :].T
            for n in range(len(cturn)):
                matches(n)

        def lse(got):
            p = jnp.max(got, axis=0)
            return p + jnp.log(jnp.sum(jnp.exp2(got - p), axis=0)) * LOG2E

        with scope("wait_stats"):
            whole(cgot.at[l, pl.ds(0, 2 * nz - 1)], ssc, rsc.at[l]).wait_recv()
            whole(rgot.at[l, pl.ds(0, nx * ny - 1)], ssr, rsr.at[l]).wait_recv()
        with scope("spread"):
            CW[...] = jnp.exp2(csend[...] - lse(cgot[l]))
            RW[...] = jnp.exp2(rsend[...] - lse(rgot[l]))
            for n, turn in enumerate(cturn):
                b = lax.rem(zh + turn, len(cturn))
                for j in range(lanes):
                    w = to_rows(CW[pl.ds(b * lanes + j, 1), :], same)
                    b1, b2 = split2(B[l, chunk(b * lanes + j, 128), :] * w)
                    BC[n, j * 128 : (j + 1) * 128, 0:128] = b1
                    BC[n, j * 128 : (j + 1) * 128, 128:256] = b2
            first = lax.broadcasted_iota(jnp.int32, (16, 128), 0)
            for n in range(rows // 128):
                cut = pl.ds(n * 128, 128)
                v = RW[n : n + 1, :]
                t1, t2 = split2(AF[:, cut] * v)
                AT[0:128, cut] = t2
                AT[128:256, cut] = t1
                low = v - v.astype(BF16).astype(F32)
                AT[256:272, cut] = jnp.where(
                    first == 0, v, jnp.where(first == 1, low, 0.0)
                ).astype(BF16)
                RB[cut, :] = jnp.broadcast_to(to_rows(v, same), (128, 128))

        def to_second(n):
            q = dot(AT[...], MH[n])
            u = dot(AT[128:272, :], ML[n])
            b = lax.rem(zh + cturn[n], len(cturn))
            w = column_line(CW, b)
            mass = (q[256:257] + q[257:258] + u[128:129] + u[129:130]) * w
            q = (q[0:128] + q[128:256] + u[0:128]) * w
            for j in range(lanes):
                t = q[:, j * 128 : (j + 1) * 128].T
                for e in range(2):
                    QS[(b * lanes + j) * 2 + e, 0:blk, :] = t[e * blk : (e + 1) * blk]
                    QS[(b * lanes + j) * 2 + e, blk:pad, :] = jnp.broadcast_to(
                        mass[:, j * 128 : (j + 1) * 128], (pad - blk, 128)
                    )

        def turned(n):
            return lax.rem(zh + cturn[n], len(cturn))

        def cross(n):
            for j in range(lanes):
                pz = turned(n) * lanes + j
                send(QS.at[pz * 2 + (1 - k)], QX.at[l, pz], sx, rx.at[l, turned(n)], sibling)

        def join(n):
            b = turned(n)
            whole(QX.at[l, pl.ds(b * lanes, lanes)], sx, rx.at[l, b]).wait_recv()
            for pz in [b * lanes, b * lanes + 1] if cturn[n] else [b * lanes + 1 - zl]:
                QS[pz * 2 + k] = QS[pz * 2 + k] + QX[l, pz]
                send(QS.at[pz * 2 + k], QR.at[l, z], sq, rq.at[l], at(x, y, pz, k))
            if not cturn[n]:
                QR[l, z] = QS[z * 2 + k] + QX[l, z]

        def to_first(n):
            at_ = chunk(lax.rem(x + rturn[n], len(rturn)), rchunk)
            b = lax.rem(x + rturn[n], len(rturn))
            p = sum(dot(MH[j, at_, :], BC[j]) for j in range(len(cturn)))
            p = p[:, 0:128] + p[:, 128:256]
            p = p + sum(dot(ML[j, at_, :], BC[j, :, 0:128]) for j in range(len(cturn)))
            p = p * RB[at_, :]
            for i in range(0, rchunk, 64):
                r = chunk(b * (rchunk // 64) + i // 64, 64)
                parts = []
                for j, turn in enumerate(cturn):
                    w = column_line(CW, lax.rem(zh + turn, len(cturn)))
                    e = E[j, r, :] * w
                    parts += [e[:, m * 128 : (m + 1) * 128] for m in range(lanes)]
                RM[r, :] = functools.reduce(jnp.add, parts) * RB[r, :]
            mass = jnp.sum(RM[at_, :], axis=1, keepdims=True)
            for e in range(ny):
                PS[b * ny + e, 0:blk, :] = p[e * blk : (e + 1) * blk]
                PS[b * ny + e, blk:pad, :] = jnp.broadcast_to(
                    to_lanes(mass[e * blk : (e + 1) * blk], small), (pad - blk, 128)
                )

        with scope("messages"):
            for n in range(max(len(cturn), len(rturn))):
                if n < len(cturn):
                    with scope("second"):
                        to_second(n)
                    cross(n)
                if n < len(rturn):
                    with scope("first"):
                        to_first(n)
                    for dy in range(ny - 1, -1, -1):
                        if (rturn[n], dy) != (0, 0):
                            s, dev = plane((rturn[n], dy))
                            send(PS.at[s], PR.at[l, me_a], sp, rp.at[l], dev)
                if n < len(cturn):
                    with scope("join"):
                        join(n)
            PR[l, me_a] = PS[me_a]

        with scope("wait_q"):
            whole(QR.at[l, pl.ds(0, nz - 1)], sq, rq.at[l]).wait_recv()
        q = jnp.sum(QR[l], axis=0)
        qm = to_rows(q[blk : blk + 1], eye(blk, lax.rem(me_b, 2) * blk))
        hy = B[l, slot(me_b), :] + q[0:blk] / (qm + offset)
        with scope("wait_p"):
            whole(PR.at[l, pl.ds(0, nx * ny - 1)], sp, rp.at[l]).wait_recv()
        with scope("refine"):
            p = jnp.sum(PR[l], axis=0)
            pm = to_rows(p[blk : blk + 1], small)
            hx = A[l, slot(me_a), :] + p[0:blk] / (pm + offset)
            h = jnp.concatenate([hx, hy], axis=0)
            scale = lax.rsqrt(jnp.mean(h * h, axis=1, keepdims=True) + 1e-05)
            u = high(h * scale * gain[pl.ds(l, 1), :], up[l]) + bias[pl.ds(l, 1), :]
            g = 0.5 * u * (1.0 + jnp.tanh(math.sqrt(2 / math.pi) * (u + 0.044715 * (u * u * u))))
            h = h + high(g, down[l])
            A[l + 1, slot(me_a), :] = h[0:blk]
            B[l + 1, slot(me_b), :] = h[blk : 2 * blk]
        with scope("drain"):
            for ref, s in [
                (A.at[l, pl.ds(0, rows - blk)], sa), (B.at[l, pl.ds(0, cols - blk)], sb),
                (cgot.at[l, pl.ds(0, 2 * nz - 1)], ssc), (rgot.at[l, pl.ds(0, nx * ny - 1)], ssr),
                (PR.at[l, pl.ds(0, nx * ny - 1)], sp), (QX.at[l], sx), (QR.at[l, pl.ds(0, nz - 1)], sq),
            ]:
                whole(ref, s, rq.at[l]).wait_send()
        return carry

    L = wq.shape[0]
    lax.fori_loop(0, L, layer, 0)
    with scope("exit"):
        last = [
            pltpu.make_async_copy(A.at[L, slot(me_a)], out.at[0], sl.at[0]),
            pltpu.make_async_copy(B.at[L, slot(me_b)], out.at[1], sl.at[1]),
        ]
        for c in last:
            c.start()
        for c in last:
            c.wait()


def align_all(dims, x, y, *weights):
    nx, ny, nz = dims
    ga, gb = nx * ny, nz * 2
    blk, d = x.shape
    rows, cols = ga * blk, gb * blk
    L = weights[0].shape[0]
    pad = blk + 8
    V, dma = pltpu.VMEM, lambda *s: pltpu.SemaphoreType.DMA(s)
    body = functools.partial(kernel, dims, blk * ga * gb)
    h = pl.pallas_call(
        body,
        out_shape=jax.ShapeDtypeStruct((2, blk, d), F32),
        in_specs=[pl.BlockSpec(memory_space=pl.ANY)] * 8,
        out_specs=pl.BlockSpec(memory_space=pl.ANY),
        scratch_shapes=[
            V((L + 1, rows, d), F32), V((L + 1, cols, d), F32), V((rows, cols), F32), V((cols // 256, rows, 256), F32),
            V((cols // 256, rows, 256), BF16), V((cols // 256, rows, 256), BF16),
            V((rows, 2 * d), BF16), V((rows, 2 * d), BF16),
            V((cols, 2 * d), BF16), V((cols, 2 * d), BF16), V((cols, 2 * d), BF16),
            V((d, rows), F32), V((2 * d + 16, rows), BF16), V((cols // 256, 256, 2 * d), BF16),
            V((rows, 128), F32), V((rows, 128), F32), V((rows, 128), F32),
            V((rows // 128, 128), F32), V((cols // 128, 128), F32),
            V((rows // 128, 128), F32), V((cols // 128, 128), F32),
            V((L, ga, rows // 128, 128), F32), V((L, gb, cols // 128, 128), F32),
            V((ga, pad, d), F32), V((L, ga, pad, d), F32),
            V((gb, pad, d), F32), V((L, nz, pad, d), F32), V((L, nz, pad, d), F32),
            *[V(w.shape, F32) for w in weights],
            dma(8), dma(L), dma(L), dma(L), dma(L, nz), *[dma(L)] * 8, dma(L, cols // 256), dma(L), dma(L),
        ],
        compiler_params=pltpu.CompilerParams(
            collective_id=0, has_side_effects=True, vmem_limit_bytes=66_000_000
        ),
    )(x, y, *weights)
    return h[0], h[1]


def solution(mesh):
    size = mesh.shape["row"] * mesh.shape["col"]
    dims = (4, 4, 8) if size == 256 else (2, 2, 2)
    placed = (P(("row", "col"), None), P(("row", "col"), None), P(), P(), P(), P(), P(), P())
    return jax.shard_map(
        functools.partial(align_all, dims),
        mesh=mesh,
        in_specs=placed,
        out_specs=(P(("row", "col"), None), P(("row", "col"), None)),
        check_vma=False,
    )
```

```python
import functools
import math

import jax
import jax.numpy as jnp
from jax import lax
from jax.experimental import pallas as pl
from jax.experimental.pallas import tpu as pltpu
from jax.sharding import PartitionSpec as P

MESH = pl.DeviceIdType.MESH
F32, BF16 = jnp.float32, jnp.bfloat16
HIGH = lax.Precision.HIGHEST
LOG2E = math.log2(math.e)
NT = (((1,), (1,)), ((), ()))


def dot(a, b, dims=(((1,), (0,)), ((), ()))):
    return lax.dot_general(a, b, dims, preferred_element_type=F32)


def high(a, b, dims=(((1,), (0,)), ((), ()))):
    return lax.dot_general(a, b, dims, precision=HIGH, preferred_element_type=F32)


def split2(v):
    top = v.astype(BF16)
    return top, (v - top.astype(F32)).astype(BF16)


def split3(v):
    top = v.astype(BF16)
    rest = v - top.astype(F32)
    mid = rest.astype(BF16)
    return top, mid, (rest - mid.astype(F32)).astype(BF16)


def eye(rows, shift=0):
    r = lax.broadcasted_iota(jnp.int32, (rows, 128), 0)
    c = lax.broadcasted_iota(jnp.int32, (rows, 128), 1)
    return c == r + shift


def to_lanes(column, mask):
    spread = jnp.broadcast_to(column, mask.shape)
    return jnp.sum(jnp.where(mask, spread, 0.0), axis=0, keepdims=True)


def to_rows(line, mask):
    spread = jnp.broadcast_to(line, mask.shape)
    return jnp.sum(jnp.where(mask, spread, 0.0), axis=1, keepdims=True)


def kernel(
    dims, total, x_ref, y_ref, wq_h, wk_h, gain_h, up_h, bias_h, down_h, out,
    A, B, S, E, MH, ML, T1, T2, K1, K2, K3, AF, AT, BC, RM, RS, RB, RW, CW,
    rsend, csend, rgot, cgot, PS, PR, QS, QX, QR,
    wq, wk, gain, up, bias, down,
    sl, sa, ra_, sb, rb_, rf, ssr, rsr, ssc, rsc, sp, rp, sx, rx, sq, rq,
):
    nx, ny, nz = dims
    row, col = lax.axis_index("row"), lax.axis_index("col")
    x, zl, k = lax.div(row, 4), lax.rem(lax.div(row, 2), 2), lax.rem(row, 2)
    zh, y = lax.div(col, ny), lax.rem(col, ny)
    z = zh * 2 + zl
    me_a, me_b = x * ny + y, z * 2 + k
    blk = x_ref.shape[0]
    rows, cols = nx * ny * blk, nz * 2 * blk
    cchunk, schunk = 256, min(256, rows)
    lanes = cchunk // 128
    offset = 0.05 / total
    factor = 2.0 / math.sqrt(x_ref.shape[1]) * LOG2E
    scope = jax.named_scope

    def at(x, y, z, k):
        return (x * 4 + lax.rem(z, 2) * 2 + k, lax.div(z, 2) * ny + y)

    def plane(n):
        px, py = lax.rem(x + n[0], nx), lax.rem(y + n[1], ny)
        return px * ny + py, at(px, py, z, k)

    def line(dz, other):
        pz = lax.rem(z + dz, nz)
        pk = 1 - k if other else k
        return pz * 2 + pk, at(x, y, pz, pk)

    near = lambda d, n: min(d, n - d)
    plane_steps = sorted(
        [(dx, dy) for dx in range(nx) for dy in range(ny) if (dx, dy) != (0, 0)],
        key=lambda s: -near(s[0], nx) - near(s[1], ny),
    )
    z_steps = sorted(range(1, nz), key=lambda d: near(d, nz))
    line_steps = [(d, o) for d in [*z_steps[::-1], 0] for o in (False, True) if (d, o) != (0, False)]
    _, sibling = line(0, True)

    def copy(src, dst, ss, rs, dev):
        return pltpu.make_async_remote_copy(
            src_ref=src, dst_ref=dst, send_sem=ss, recv_sem=rs, device_id=dev, device_id_type=MESH
        )

    def slot(n):
        return pl.ds(pl.multiple_of(n * blk, blk), blk)

    def chunk(n, size):
        return pl.ds(pl.multiple_of(n * size, size), size)

    with scope("entry"):
        barrier = pltpu.get_barrier_semaphore()
        for step in plane_steps:
            pl.semaphore_signal(barrier, inc=1, device_id=plane(step)[1], device_id_type=MESH)
        for step in line_steps:
            pl.semaphore_signal(barrier, inc=1, device_id=line(*step)[1], device_id_type=MESH)
        moves = [
            (x_ref, A.at[0, slot(me_a)]), (y_ref, B.at[0, slot(me_b)]), (wq_h, wq), (wk_h, wk),
            (gain_h, gain), (up_h, up), (bias_h, bias), (down_h, down),
        ]
        moves = [pltpu.make_async_copy(a, b, sl.at[n]) for n, (a, b) in enumerate(moves)]
        for m in moves:
            m.start()
        for m in moves[:2]:
            m.wait()
        pl.semaphore_wait(barrier, len(plane_steps) + len(line_steps))

    same, small = eye(128), eye(blk)

    def layer(l, carry):
        def send(src, dst, ss, rs, dev):
            copy(src, dst, ss.at[l], rs, dev).start()

        def whole(ref, ss, rs):
            return copy(ref, ref, ss.at[l], rs, sibling)

        own_a, own_b = A.at[l, slot(me_a)], B.at[l, slot(me_b)]
        send(own_b, own_b, sb, rf.at[l], sibling)
        for n, d in enumerate(z_steps[::-1]):
            send(own_b, own_b, sb, rb_.at[l, z], line(d, False)[1])
        for n, step in enumerate(plane_steps):
            send(own_a, own_a, sa, ra_.at[l], plane(step)[1])

        @pl.when(l == 0)
        def _():
            for m in moves[2:]:
                m.wait()

        m1, m2, m3 = split3(high(wk[l], wq[l], NT) * factor)
        stack = lambda a, b: jnp.concatenate([a, b], axis=0)
        mix_a = jnp.concatenate([stack(m1, m2), stack(m2, m1)], axis=1)
        mix_b = stack(m3, m1)

        def make_keys(at_):
            b1, b2, b3 = split3(B[l, at_, :])
            t = dot(jnp.concatenate([b1, b2], axis=1), mix_a)
            t = t[:, 0:128] + (t[:, 128:256] + dot(jnp.concatenate([b1, b3], axis=1), mix_b))
            k1, k2, k3 = split3(t)
            K1[at_, 0:128] = k1
            K1[at_, 128:256] = k2
            K2[at_, 0:128] = k2
            K2[at_, 128:256] = k1
            K3[at_, 0:128] = k3
            K3[at_, 128:256] = k1

        def make_rows(at_):
            a1, a2, a3 = split3(A[l, at_, :])
            T1[at_, 0:128] = a1
            T1[at_, 128:256] = a2
            T2[at_, 0:128] = a1
            T2[at_, 128:256] = a3

        with scope("gather"):
            for d in z_steps[::-1]:
                s, _ = line(d, False)
                ref, pz = B.at[l, slot(s)], lax.rem(z + d, nz)
                whole(ref, sb, rb_.at[l, pz]).wait_recv()
                send(ref, ref, sb, rf.at[l], sibling)
            whole(A.at[l, pl.ds(0, rows - blk)], sa, ra_.at[l]).wait_recv()
            whole(B.at[l, pl.ds(0, cols // 2)], sb, rf.at[l]).wait_recv()
        with scope("operands"):
            for n in range(cols // 256):
                make_keys(pl.ds(n * 256, 256))
            for n in range(rows // 256):
                make_rows(pl.ds(n * 256, 256))

        def product(n):
            at_ = pl.ds(n * schunk, schunk)
            t1, t2 = T1[at_, :], T2[at_, :]
            S[at_, :] = dot(t1, K1[...], NT) + dot(t1, K2[...], NT) + dot(t2, K3[...], NT)

        def row_statistics(n):
            for i in range(n * schunk, (n + 1) * schunk, 8):
                r = pl.ds(i, 8)
                parts = [S[r, j * 128 : (j + 1) * 128] for j in range(cols // 128)]
                m = functools.reduce(jnp.maximum, parts)
                RM[r, :] = m
                RS[r, :] = functools.reduce(jnp.add, [jnp.exp2(p - m) for p in parts])
            for i in range(n * schunk, (n + 1) * schunk, 128):
                at_ = pl.ds(i, 128)
                m = RM[at_, :]
                p = jnp.max(m, axis=1, keepdims=True)
                t = jnp.sum(RS[at_, :] * jnp.exp2(m - p), axis=1, keepdims=True)
                own = jnp.broadcast_to(p + jnp.log(t) * LOG2E, (128, 128))
                RB[at_, :] = own
                rsend[i // 128 : i // 128 + 1, :] = to_lanes(own, same)

        def column_statistics(j):
            at_ = pl.ds(j * cchunk, cchunk)
            m = [S[i * 8 : (i + 1) * 8, at_] for i in range(4)]
            for i in range(32, rows, 32):
                m = [jnp.maximum(m[e], S[i + e * 8 : i + e * 8 + 8, at_]) for e in range(4)]
            p = jnp.max(functools.reduce(jnp.maximum, m), axis=0, keepdims=True)
            pb = jnp.broadcast_to(p, (8, cchunk))
            t = [jnp.zeros((8, cchunk), F32)] * 4
            for i in range(0, rows, 32):
                t = [t[e] + jnp.exp2(S[i + e * 8 : i + e * 8 + 8, at_] - pb) for e in range(4)]
            c = p + jnp.log(jnp.sum(functools.reduce(jnp.add, t), axis=0, keepdims=True)) * LOG2E
            for e in range(lanes):
                csend[j * lanes + e : j * lanes + e + 1, :] = c[:, e * 128 : (e + 1) * 128]

        with scope("score"):
            product(0)
            for n in range(rows // schunk):
                if n + 1 < rows // schunk:
                    product(n + 1)
                row_statistics(n)
            for n, step in enumerate(plane_steps):
                send(rsend, rgot.at[l, me_a], ssr, rsr.at[l], plane(step)[1])
        with scope("lse"):
            for j in range(cols // cchunk):
                column_statistics(j)
            for n, step in enumerate(line_steps):
                send(csend, cgot.at[l, me_b], ssc, rsc.at[l], line(*step)[1])
        cgot[l, me_b] = csend[...]
        rgot[l, me_a] = rsend[...]
        turns = {4: (2, 1, 3, 0), 2: (1, 0), 1: (0,)}
        cturn = turns[cols // cchunk]
        parcels = {
            4: [
                [(2, 2), (2, 0), (0, 2), (1, 1)], [(1, 2), (3, 2), (2, 1), (2, 3)],
                [(1, 3), (3, 1), (3, 3), (1, 0)], [(3, 0), (0, 1), (0, 3), (0, 0)],
            ],
            2: [[(1, 1), (1, 0), (0, 1), (0, 0)]],
        }[nx]
        body = pl.ds(0, blk + 1)

        def column_line(ref, b):
            return jnp.concatenate([ref[pl.ds(b * lanes + j, 1), :] for j in range(lanes)], axis=1)

        def matches(n):
            b = lax.rem(zh + cturn[n], len(cturn))
            at_ = chunk(b, cchunk)
            cb = jnp.broadcast_to(column_line(csend, b), (16, cchunk))
            for i in range(0, rows, 16):
                r = pl.ds(i, 16)
                s = S[r, at_]
                rb = RB[r, :]
                m = jnp.exp2((s - jnp.concatenate([rb] * lanes, axis=1)) + (s - cb))
                E[n, r, :] = m
                h, lo = split2(m)
                MH[n, r, :] = h
                ML[n, r, :] = lo

        with scope("match"):
            for n in range(rows // 128):
                AF[:, n * 128 : (n + 1) * 128] = A[l, n * 128 : (n + 1) * 128, :].T
            for n in range(len(cturn)):
                matches(n)

        def lse(got):
            p = jnp.max(got, axis=0)
            return p + jnp.log(jnp.sum(jnp.exp2(got - p), axis=0)) * LOG2E

        with scope("wait_rows"):
            whole(rgot.at[l, pl.ds(0, nx * ny - 1)], ssr, rsr.at[l]).wait_recv()
        with scope("spread"):
            RW[...] = jnp.exp2(rsend[...] - lse(rgot[l]))
            first = lax.broadcasted_iota(jnp.int32, (16, 128), 0)
            for n in range(rows // 128):
                cut = pl.ds(n * 128, 128)
                v = RW[n : n + 1, :]
                t1, t2 = split2(AF[:, cut] * v)
                AT[0:128, cut] = t2
                AT[128:256, cut] = t1
                low = v - v.astype(BF16).astype(F32)
                AT[256:272, cut] = jnp.where(
                    first == 0, v, jnp.where(first == 1, low, 0.0)
                ).astype(BF16)

        def column_weights():
            with scope("wait_columns"):
                whole(cgot.at[l, pl.ds(0, 2 * nz - 1)], ssc, rsc.at[l]).wait_recv()
            CW[...] = jnp.exp2(csend[...] - lse(cgot[l]))

        def first_operands():
            with scope("spread"):
                for n, turn in enumerate(cturn):
                    b = lax.rem(zh + turn, len(cturn))
                    for j in range(lanes):
                        w = to_rows(CW[pl.ds(b * lanes + j, 1), :], same)
                        b1, b2 = split2(B[l, chunk(b * lanes + j, 128), :] * w)
                        BC[n, j * 128 : (j + 1) * 128, 0:128] = b1
                        BC[n, j * 128 : (j + 1) * 128, 128:256] = b2
                for n in range(rows // 128):
                    RB[n * 128 : (n + 1) * 128, :] = jnp.broadcast_to(
                        to_rows(RW[n : n + 1, :], same), (128, 128)
                    )

        def to_second(n):
            q = dot(AT[...], MH[n])
            u = dot(AT[128:272, :], ML[n])
            if n == 0:
                column_weights()
            b = lax.rem(zh + cturn[n], len(cturn))
            w = column_line(CW, b)
            mass = (q[256:257] + q[257:258] + u[128:129] + u[129:130]) * w
            q = (q[0:128] + q[128:256] + u[0:128]) * w
            for j in range(lanes):
                t = q[:, j * 128 : (j + 1) * 128].T
                for e in range(2):
                    QS[(b * lanes + j) * 2 + e, 0:blk, :] = t[e * blk : (e + 1) * blk]
                    QS[(b * lanes + j) * 2 + e, blk : blk + 1, :] = mass[:, j * 128 : (j + 1) * 128]

        def turned(n):
            return lax.rem(zh + cturn[n], len(cturn))

        def cross(n):
            for j in range(lanes):
                pz = turned(n) * lanes + j
                send(QS.at[pz * 2 + (1 - k), body], QX.at[l, pz, body], sx, rx.at[l, turned(n)], sibling)

        def join(n):
            b = turned(n)
            whole(QX.at[l, pl.ds(b * lanes, lanes), body], sx, rx.at[l, b]).wait_recv()
            for pz in [b * lanes, b * lanes + 1] if cturn[n] else [b * lanes + 1 - zl]:
                QS[pz * 2 + k, body] = QS[pz * 2 + k, body] + QX[l, pz, body]
                send(QS.at[pz * 2 + k, body], QR.at[l, z, body], sq, rq.at[l], at(x, y, pz, k))
            if not cturn[n]:
                QR[l, z, body] = QS[z * 2 + k, body] + QX[l, z, body]

        def to_first(n):
            owners = [plane(o)[0] for o in parcels[n]]
            left = lambda ref: jnp.concatenate([ref[slot(s), :] for s in owners], axis=0)
            p = sum(dot(left(MH.at[j]), BC[j]) for j in range(len(cturn)))
            p = p[:, 0:128] + p[:, 128:256]
            p = p + sum(dot(left(ML.at[j]), BC[j, :, 0:128]) for j in range(len(cturn)))
            for e, s in enumerate(owners):
                parts = []
                for j, turn in enumerate(cturn):
                    w = column_line(CW, lax.rem(zh + turn, len(cturn)))
                    t = E[j, slot(s), :] * w
                    parts += [t[:, m * 128 : (m + 1) * 128] for m in range(lanes)]
                v = RB[slot(s), :]
                mass = jnp.sum(functools.reduce(jnp.add, parts) * v, axis=1, keepdims=True)
                PS[s, 0:blk, :] = p[e * blk : (e + 1) * blk] * v
                PS[s, blk : blk + 1, :] = to_lanes(mass, small)

        def give(n):
            to_first(n)
            for o in parcels[n]:
                s, dev = plane(o)
                if o != (0, 0):
                    send(PS.at[s, body], PR.at[l, me_a, body], sp, rp.at[l], dev)
                else:
                    PR[l, me_a, body] = PS[me_a, body]

        with scope("messages"):
            def second(n):
                with scope("second"):
                    to_second(n)
                cross(n)
                if n == 0:
                    first_operands()

            def first(n):
                with scope("first"):
                    give(n)

            def joined(n):
                with scope("join"):
                    join(n)

            if len(cturn) == 4:
                for f, n in zip(
                    (second, first, joined, second, second, joined, first, second, joined, first, joined, first),
                    (0, 0, 0, 1, 2, 1, 1, 3, 2, 2, 3, 3),
                ):
                    f(n)
            else:
                for n in range(len(cturn)):
                    second(n)
                    joined(n)
                for n in range(len(parcels)):
                    first(n)

        with scope("wait_q"):
            whole(QR.at[l, pl.ds(0, nz - 1), body], sq, rq.at[l]).wait_recv()
        q = jnp.sum(QR[l, :, body], axis=0)
        qm = to_rows(q[blk : blk + 1], eye(blk, lax.rem(me_b, 2) * blk))
        hy = B[l, slot(me_b), :] + q[0:blk] / (qm + offset)
        with scope("wait_p"):
            whole(PR.at[l, pl.ds(0, nx * ny - 1), body], sp, rp.at[l]).wait_recv()
        with scope("refine"):
            p = jnp.sum(PR[l, :, body], axis=0)
            pm = to_rows(p[blk : blk + 1], small)
            hx = A[l, slot(me_a), :] + p[0:blk] / (pm + offset)
            h = jnp.concatenate([hx, hy], axis=0)
            scale = lax.rsqrt(jnp.mean(h * h, axis=1, keepdims=True) + 1e-05)
            u = high(h * scale * gain[pl.ds(l, 1), :], up[l]) + bias[pl.ds(l, 1), :]
            g = 0.5 * u * (1.0 + jnp.tanh(math.sqrt(2 / math.pi) * (u + 0.044715 * (u * u * u))))
            h = h + high(g, down[l])
            A[l + 1, slot(me_a), :] = h[0:blk]
            B[l + 1, slot(me_b), :] = h[blk : 2 * blk]
        with scope("drain"):
            for ref, s in [
                (A.at[l, pl.ds(0, rows - blk)], sa), (B.at[l, pl.ds(0, cols - blk)], sb),
                (cgot.at[l, pl.ds(0, 2 * nz - 1)], ssc), (rgot.at[l, pl.ds(0, nx * ny - 1)], ssr),
                (PR.at[l, pl.ds(0, nx * ny - 1), body], sp), (QX.at[l, :, body], sx),
                (QR.at[l, pl.ds(0, nz - 1), body], sq),
            ]:
                whole(ref, s, rq.at[l]).wait_send()
        return carry

    L = wq.shape[0]
    lax.fori_loop(0, L, layer, 0)
    with scope("exit"):
        last = [
            pltpu.make_async_copy(A.at[L, slot(me_a)], out.at[0], sl.at[0]),
            pltpu.make_async_copy(B.at[L, slot(me_b)], out.at[1], sl.at[1]),
        ]
        for c in last:
            c.start()
        for c in last:
            c.wait()


def align_all(dims, x, y, *weights):
    nx, ny, nz = dims
    ga, gb = nx * ny, nz * 2
    blk, d = x.shape
    rows, cols = ga * blk, gb * blk
    L = weights[0].shape[0]
    pad = blk + 8
    V, dma = pltpu.VMEM, lambda *s: pltpu.SemaphoreType.DMA(s)
    body = functools.partial(kernel, dims, blk * ga * gb)
    h = pl.pallas_call(
        body,
        out_shape=jax.ShapeDtypeStruct((2, blk, d), F32),
        in_specs=[pl.BlockSpec(memory_space=pl.ANY)] * 8,
        out_specs=pl.BlockSpec(memory_space=pl.ANY),
        scratch_shapes=[
            V((L + 1, rows, d), F32), V((L + 1, cols, d), F32), V((rows, cols), F32), V((cols // 256, rows, 256), F32),
            V((cols // 256, rows, 256), BF16), V((cols // 256, rows, 256), BF16),
            V((rows, 2 * d), BF16), V((rows, 2 * d), BF16),
            V((cols, 2 * d), BF16), V((cols, 2 * d), BF16), V((cols, 2 * d), BF16),
            V((d, rows), F32), V((2 * d + 16, rows), BF16), V((cols // 256, 256, 2 * d), BF16),
            V((rows, 128), F32), V((rows, 128), F32), V((rows, 128), F32),
            V((rows // 128, 128), F32), V((cols // 128, 128), F32),
            V((rows // 128, 128), F32), V((cols // 128, 128), F32),
            V((L, ga, rows // 128, 128), F32), V((L, gb, cols // 128, 128), F32),
            V((ga, pad, d), F32), V((L, ga, pad, d), F32),
            V((gb, pad, d), F32), V((L, nz, pad, d), F32), V((L, nz, pad, d), F32),
            *[V(w.shape, F32) for w in weights],
            dma(8), dma(L), dma(L), dma(L), dma(L, nz), *[dma(L)] * 8, dma(L, cols // 256), dma(L), dma(L),
        ],
        compiler_params=pltpu.CompilerParams(
            collective_id=0, has_side_effects=True, vmem_limit_bytes=66_000_000
        ),
    )(x, y, *weights)
    return h[0], h[1]


def solution(mesh):
    size = mesh.shape["row"] * mesh.shape["col"]
    dims = (4, 4, 8) if size == 256 else (2, 2, 2)
    placed = (P(("row", "col"), None), P(("row", "col"), None), P(), P(), P(), P(), P(), P())
    return jax.shard_map(
        functools.partial(align_all, dims),
        mesh=mesh,
        in_specs=placed,
        out_specs=(P(("row", "col"), None), P(("row", "col"), None)),
        check_vma=False,
    )
```

```python
import functools
import math

import jax
import jax.numpy as jnp
from jax import lax
from jax.experimental import pallas as pl
from jax.experimental.pallas import tpu as pltpu
from jax.sharding import PartitionSpec as P

MESH = pl.DeviceIdType.MESH
F32, BF16 = jnp.float32, jnp.bfloat16
HIGH = lax.Precision.HIGHEST
LOG2E = math.log2(math.e)
NT = (((1,), (1,)), ((), ()))


def dot(a, b, dims=(((1,), (0,)), ((), ()))):
    return lax.dot_general(a, b, dims, preferred_element_type=F32)


def high(a, b, dims=(((1,), (0,)), ((), ()))):
    return lax.dot_general(a, b, dims, precision=HIGH, preferred_element_type=F32)


def split2(v):
    top = v.astype(BF16)
    return top, (v - top.astype(F32)).astype(BF16)


def split3(v):
    top = v.astype(BF16)
    rest = v - top.astype(F32)
    mid = rest.astype(BF16)
    return top, mid, (rest - mid.astype(F32)).astype(BF16)


def eye(rows, shift=0):
    r = lax.broadcasted_iota(jnp.int32, (rows, 128), 0)
    c = lax.broadcasted_iota(jnp.int32, (rows, 128), 1)
    return c == r + shift


def to_lanes(column, mask):
    spread = jnp.broadcast_to(column, mask.shape)
    return jnp.sum(jnp.where(mask, spread, 0.0), axis=0, keepdims=True)


def to_rows(line, mask):
    spread = jnp.broadcast_to(line, mask.shape)
    return jnp.sum(jnp.where(mask, spread, 0.0), axis=1, keepdims=True)


def kernel(
    dims, total, x_ref, y_ref, wq_h, wk_h, gain_h, up_h, bias_h, down_h, out,
    A, B, S, E, MH, ML, T1, T2, K1, K2, K3, AF, AT, BC, RM, RS, RB, RW, CW,
    rsend, csend, rgot, cgot, PS, PR, QS, QX, QR,
    wq, wk, gain, up, bias, down, U, W,
    sl, sa, ra_, sb, rb_, rf, ssr, rsr, ssc, rsc, sp, rp, sx, rx, sq, rq,
):
    nx, ny, nz = dims
    row, col = lax.axis_index("row"), lax.axis_index("col")
    x, zl, k = lax.div(row, 4), lax.rem(lax.div(row, 2), 2), lax.rem(row, 2)
    zh, y = lax.div(col, ny), lax.rem(col, ny)
    z = zh * 2 + zl
    me_a, me_b = x * ny + y, z * 2 + k
    blk = x_ref.shape[0]
    rows, cols = nx * ny * blk, nz * 2 * blk
    cchunk, schunk = 256, min(256, rows)
    lanes = cchunk // 128
    offset = 0.05 / total
    factor = 2.0 / math.sqrt(x_ref.shape[1]) * LOG2E
    scope = jax.named_scope

    def at(x, y, z, k):
        return (x * 4 + lax.rem(z, 2) * 2 + k, lax.div(z, 2) * ny + y)

    def plane(n):
        px, py = lax.rem(x + n[0], nx), lax.rem(y + n[1], ny)
        return px * ny + py, at(px, py, z, k)

    def line(dz, other):
        pz = lax.rem(z + dz, nz)
        pk = 1 - k if other else k
        return pz * 2 + pk, at(x, y, pz, pk)

    near = lambda d, n: min(d, n - d)
    plane_steps = sorted(
        [(dx, dy) for dx in range(nx) for dy in range(ny) if (dx, dy) != (0, 0)],
        key=lambda s: -near(s[0], nx) - near(s[1], ny),
    )
    z_steps = sorted(range(1, nz), key=lambda d: near(d, nz))
    line_steps = [(d, o) for d in [*z_steps[::-1], 0] for o in (False, True) if (d, o) != (0, False)]
    _, sibling = line(0, True)

    def copy(src, dst, ss, rs, dev):
        return pltpu.make_async_remote_copy(
            src_ref=src, dst_ref=dst, send_sem=ss, recv_sem=rs, device_id=dev, device_id_type=MESH
        )

    def slot(n):
        return pl.ds(pl.multiple_of(n * blk, blk), blk)

    def chunk(n, size):
        return pl.ds(pl.multiple_of(n * size, size), size)

    with scope("entry"):
        barrier = pltpu.get_barrier_semaphore()
        for step in plane_steps:
            pl.semaphore_signal(barrier, inc=1, device_id=plane(step)[1], device_id_type=MESH)
        for step in line_steps:
            pl.semaphore_signal(barrier, inc=1, device_id=line(*step)[1], device_id_type=MESH)
        moves = [
            (x_ref, A.at[0, slot(me_a)]), (y_ref, B.at[0, slot(me_b)]), (wq_h, wq), (wk_h, wk),
            (gain_h, gain), (up_h, up), (bias_h, bias), (down_h, down),
        ]
        moves = [pltpu.make_async_copy(a, b, sl.at[n]) for n, (a, b) in enumerate(moves)]
        for m in moves:
            m.start()
        for m in moves[:2]:
            m.wait()
        pl.semaphore_wait(barrier, len(plane_steps) + len(line_steps))

    same, small = eye(128), eye(blk)

    def layer(l, carry):
        def send(src, dst, ss, rs, dev):
            copy(src, dst, ss.at[l], rs, dev).start()

        def whole(ref, ss, rs):
            return copy(ref, ref, ss.at[l], rs, sibling)

        own_a, own_b = A.at[l, slot(me_a)], B.at[l, slot(me_b)]
        send(own_b, own_b, sb, rf.at[l], sibling)
        for n, d in enumerate(z_steps[::-1]):
            send(own_b, own_b, sb, rb_.at[l, z], line(d, False)[1])
        for n, step in enumerate(plane_steps):
            send(own_a, own_a, sa, ra_.at[l], plane(step)[1])

        @pl.when(l == 0)
        def _():
            for m in moves[2:]:
                m.wait()

        m1, m2, m3 = split3(high(wk[l], wq[l], NT) * factor)
        stack = lambda a, b: jnp.concatenate([a, b], axis=0)
        mix_a = jnp.concatenate([stack(m1, m2), stack(m2, m1)], axis=1)
        mix_b = stack(m3, m1)

        def make_keys(at_):
            b1, b2, b3 = split3(B[l, at_, :])
            t = dot(jnp.concatenate([b1, b2], axis=1), mix_a)
            t = t[:, 0:128] + (t[:, 128:256] + dot(jnp.concatenate([b1, b3], axis=1), mix_b))
            k1, k2, k3 = split3(t)
            K1[at_, 0:128] = k1
            K1[at_, 128:256] = k2
            K2[at_, 0:128] = k2
            K2[at_, 128:256] = k1
            K3[at_, 0:128] = k3
            K3[at_, 128:256] = k1

        def make_rows(at_):
            a1, a2, a3 = split3(A[l, at_, :])
            T1[at_, 0:128] = a1
            T1[at_, 128:256] = a2
            T2[at_, 0:128] = a1
            T2[at_, 128:256] = a3

        with scope("gather"):
            for n, d in enumerate(z_steps[::-1]):
                s, _ = line(d, False)
                ref, pz = B.at[l, slot(s)], lax.rem(z + d, nz)
                whole(ref, sb, rb_.at[l, pz]).wait_recv()
                send(ref, ref, sb, rf.at[l], sibling)
                if n == 0:
                    make_keys(slot(me_b))
                if n < 2:
                    make_keys(slot(s))
            with scope("operands"):
                for d in z_steps[::-1][2:]:
                    make_keys(slot(line(d, False)[0]))
            whole(A.at[l, pl.ds(0, rows - blk)], sa, ra_.at[l]).wait_recv()
            with scope("operands"):
                for n in range(rows // 256):
                    make_rows(pl.ds(n * 256, 256))
            whole(B.at[l, pl.ds(0, cols // 2)], sb, rf.at[l]).wait_recv()
            with scope("operands"):
                for n in range(nz):
                    make_keys(slot(n * 2 + 1 - k))

        def product(n):
            at_ = pl.ds(n * schunk, schunk)
            t1, t2 = T1[at_, :], T2[at_, :]
            S[at_, :] = dot(t1, K1[...], NT) + dot(t1, K2[...], NT) + dot(t2, K3[...], NT)

        def row_statistics(n):
            for i in range(n * schunk, (n + 1) * schunk, 8):
                r = pl.ds(i, 8)
                parts = [S[r, j * 128 : (j + 1) * 128] for j in range(cols // 128)]
                m = functools.reduce(jnp.maximum, parts)
                RM[r, :] = m
                RS[r, :] = functools.reduce(jnp.add, [jnp.exp2(p - m) for p in parts])
            for i in range(n * schunk, (n + 1) * schunk, 128):
                at_ = pl.ds(i, 128)
                m = RM[at_, :]
                p = jnp.max(m, axis=1, keepdims=True)
                t = jnp.sum(RS[at_, :] * jnp.exp2(m - p), axis=1, keepdims=True)
                own = jnp.broadcast_to(p + jnp.log(t) * LOG2E, (128, 128))
                RB[at_, :] = own
                rsend[i // 128 : i // 128 + 1, :] = to_lanes(own, same)

        def column_statistics(j):
            at_ = pl.ds(j * cchunk, cchunk)
            m = [S[i * 8 : (i + 1) * 8, at_] for i in range(4)]
            for i in range(32, rows, 32):
                m = [jnp.maximum(m[e], S[i + e * 8 : i + e * 8 + 8, at_]) for e in range(4)]
            p = jnp.max(functools.reduce(jnp.maximum, m), axis=0, keepdims=True)
            pb = jnp.broadcast_to(p, (8, cchunk))
            t = [jnp.zeros((8, cchunk), F32)] * 4
            for i in range(0, rows, 32):
                t = [t[e] + jnp.exp2(S[i + e * 8 : i + e * 8 + 8, at_] - pb) for e in range(4)]
            c = p + jnp.log(jnp.sum(functools.reduce(jnp.add, t), axis=0, keepdims=True)) * LOG2E
            for e in range(lanes):
                csend[j * lanes + e : j * lanes + e + 1, :] = c[:, e * 128 : (e + 1) * 128]

        with scope("score"):
            product(0)
            for n in range(rows // schunk):
                if n + 1 < rows // schunk:
                    product(n + 1)
                row_statistics(n)
            for n, step in enumerate(plane_steps):
                send(rsend, rgot.at[l, me_a], ssr, rsr.at[l], plane(step)[1])
        with scope("lse"):
            for j in range(cols // cchunk):
                column_statistics(j)
            for n, step in enumerate(line_steps):
                send(csend, cgot.at[l, me_b], ssc, rsc.at[l], line(*step)[1])
        cgot[l, me_b] = csend[...]
        rgot[l, me_a] = rsend[...]
        turns = {4: (2, 1, 3, 0), 2: (1, 0), 1: (0,)}
        cturn = turns[cols // cchunk]
        parcels = {
            4: [
                [(2, 2), (2, 0), (0, 2), (1, 1)], [(1, 2), (3, 2), (2, 1), (2, 3)],
                [(1, 3), (3, 1), (3, 3), (1, 0)], [(3, 0), (0, 1), (0, 3), (0, 0)],
            ],
            2: [[(1, 1), (1, 0), (0, 1), (0, 0)]],
        }[nx]
        body = pl.ds(0, blk + 1)

        def column_line(ref, b):
            return jnp.concatenate([ref[pl.ds(b * lanes + j, 1), :] for j in range(lanes)], axis=1)

        def matches(n):
            b = lax.rem(zh + cturn[n], len(cturn))
            at_ = chunk(b, cchunk)
            cb = jnp.broadcast_to(column_line(csend, b), (16, cchunk))
            for i in range(0, rows, 16):
                r = pl.ds(i, 16)
                s = S[r, at_]
                rb = RB[r, :]
                m = jnp.exp2((s - jnp.concatenate([rb] * lanes, axis=1)) + (s - cb))
                E[n, r, :] = m
                h, lo = split2(m)
                MH[n, r, :] = h
                ML[n, r, :] = lo

        with scope("match"):
            for n in range(rows // 128):
                AF[:, n * 128 : (n + 1) * 128] = A[l, n * 128 : (n + 1) * 128, :].T
            for n in range(len(cturn)):
                matches(n)

        def lse(got):
            p = jnp.max(got, axis=0)
            return p + jnp.log(jnp.sum(jnp.exp2(got - p), axis=0)) * LOG2E

        with scope("weights"):
            u1, u2 = split2(up[l])
            U[0, 0:128, :] = u1
            U[0, 128:256, :] = u1
            U[1, 0:128, :] = u2
            U[1, 128:256, :] = u2
            w1, w2 = split2(down[l])
            W[:, 0:128] = w1
            W[:, 128:256] = w2
        with scope("wait_rows"):
            whole(rgot.at[l, pl.ds(0, nx * ny - 1)], ssr, rsr.at[l]).wait_recv()
        with scope("spread"):
            RW[...] = jnp.exp2(rsend[...] - lse(rgot[l]))
            first = lax.broadcasted_iota(jnp.int32, (16, 128), 0)
            for n in range(rows // 128):
                cut = pl.ds(n * 128, 128)
                v = RW[n : n + 1, :]
                t1, t2 = split2(AF[:, cut] * v)
                AT[0:128, cut] = t2
                AT[128:256, cut] = t1
                low = v - v.astype(BF16).astype(F32)
                AT[256:272, cut] = jnp.where(
                    first == 0, v, jnp.where(first == 1, low, 0.0)
                ).astype(BF16)

        def column_weights():
            with scope("wait_columns"):
                whole(cgot.at[l, pl.ds(0, 2 * nz - 1)], ssc, rsc.at[l]).wait_recv()
            CW[...] = jnp.exp2(csend[...] - lse(cgot[l]))

        def first_operands():
            with scope("spread"):
                for n, turn in enumerate(cturn):
                    b = lax.rem(zh + turn, len(cturn))
                    for j in range(lanes):
                        w = to_rows(CW[pl.ds(b * lanes + j, 1), :], same)
                        b1, b2 = split2(B[l, chunk(b * lanes + j, 128), :] * w)
                        BC[n, j * 128 : (j + 1) * 128, 0:128] = b1
                        BC[n, j * 128 : (j + 1) * 128, 128:256] = b2
                for n in range(rows // 128):
                    RB[n * 128 : (n + 1) * 128, :] = jnp.broadcast_to(
                        to_rows(RW[n : n + 1, :], same), (128, 128)
                    )

        def to_second(n):
            q = dot(AT[...], MH[n])
            u = dot(AT[128:272, :], ML[n])
            if n == 0:
                column_weights()
            b = lax.rem(zh + cturn[n], len(cturn))
            w = column_line(CW, b)
            mass = (q[256:257] + q[257:258] + u[128:129] + u[129:130]) * w
            q = (q[0:128] + q[128:256] + u[0:128]) * w
            for j in range(lanes):
                t = q[:, j * 128 : (j + 1) * 128].T
                for e in range(2):
                    QS[(b * lanes + j) * 2 + e, 0:blk, :] = t[e * blk : (e + 1) * blk]
                    QS[(b * lanes + j) * 2 + e, blk : blk + 1, :] = mass[:, j * 128 : (j + 1) * 128]

        def turned(n):
            return lax.rem(zh + cturn[n], len(cturn))

        def cross(n):
            for j in range(lanes):
                pz = turned(n) * lanes + j
                send(QS.at[pz * 2 + (1 - k), body], QX.at[l, pz, body], sx, rx.at[l, turned(n)], sibling)

        def join(n):
            b = turned(n)
            whole(QX.at[l, pl.ds(b * lanes, lanes), body], sx, rx.at[l, b]).wait_recv()
            for pz in [b * lanes, b * lanes + 1] if cturn[n] else [b * lanes + 1 - zl]:
                QS[pz * 2 + k, body] = QS[pz * 2 + k, body] + QX[l, pz, body]
                send(QS.at[pz * 2 + k, body], QR.at[l, z, body], sq, rq.at[l], at(x, y, pz, k))
            if not cturn[n]:
                QR[l, z, body] = QS[z * 2 + k, body] + QX[l, z, body]

        def to_first(n):
            owners = [plane(o)[0] for o in parcels[n]]
            left = lambda ref: jnp.concatenate([ref[slot(s), :] for s in owners], axis=0)
            p = sum(dot(left(MH.at[j]), BC[j]) for j in range(len(cturn)))
            p = p[:, 0:128] + p[:, 128:256]
            p = p + sum(dot(left(ML.at[j]), BC[j, :, 0:128]) for j in range(len(cturn)))
            for e, s in enumerate(owners):
                parts = []
                for j, turn in enumerate(cturn):
                    w = column_line(CW, lax.rem(zh + turn, len(cturn)))
                    t = E[j, slot(s), :] * w
                    parts += [t[:, m * 128 : (m + 1) * 128] for m in range(lanes)]
                v = RB[slot(s), :]
                mass = jnp.sum(functools.reduce(jnp.add, parts) * v, axis=1, keepdims=True)
                PS[s, 0:blk, :] = p[e * blk : (e + 1) * blk] * v
                PS[s, blk : blk + 1, :] = to_lanes(mass, small)

        def give(n):
            to_first(n)
            for o in parcels[n]:
                s, dev = plane(o)
                if o != (0, 0):
                    send(PS.at[s, body], PR.at[l, me_a, body], sp, rp.at[l], dev)
                else:
                    PR[l, me_a, body] = PS[me_a, body]

        with scope("messages"):
            def second(n):
                with scope("second"):
                    to_second(n)
                cross(n)
                if n == 0:
                    first_operands()

            def first(n):
                with scope("first"):
                    give(n)

            def joined(n):
                with scope("join"):
                    join(n)

            if len(cturn) == 4:
                for f, n in zip(
                    (second, first, joined, second, second, joined, first, second, joined, first, joined, first),
                    (0, 0, 0, 1, 2, 1, 1, 3, 2, 2, 3, 3),
                ):
                    f(n)
            else:
                for n in range(len(cturn)):
                    second(n)
                    joined(n)
                for n in range(len(parcels)):
                    first(n)

        with scope("wait_q"):
            whole(QR.at[l, pl.ds(0, nz - 1), body], sq, rq.at[l]).wait_recv()
        q = jnp.sum(QR[l, :, body], axis=0)
        qm = to_rows(q[blk : blk + 1], eye(blk, lax.rem(me_b, 2) * blk))
        hy = B[l, slot(me_b), :] + q[0:blk] / (qm + offset)
        with scope("wait_p"):
            whole(PR.at[l, pl.ds(0, nx * ny - 1), body], sp, rp.at[l]).wait_recv()
        with scope("refine"):
            p = jnp.sum(PR[l, :, body], axis=0)
            pm = to_rows(p[blk : blk + 1], small)
            hx = A[l, slot(me_a), :] + p[0:blk] / (pm + offset)
            h = jnp.concatenate([hx, hy], axis=0)
            scale = lax.rsqrt(jnp.mean(h * h, axis=1, keepdims=True) + 1e-05)
            n1, n2 = split2(h * scale * gain[pl.ds(l, 1), :])
            n12 = jnp.concatenate([n1, n2], axis=1)
            u = dot(n12, U[0]) + dot(n12, U[1]) + bias[pl.ds(l, 1), :]
            g = 0.5 * u * (1.0 + jnp.tanh(math.sqrt(2 / math.pi) * (u + 0.044715 * (u * u * u))))
            g1, g2 = split2(g)
            t = dot(g1, W[...]) + dot(g2, W[...])
            h = h + (t[:, 0:128] + t[:, 128:256])
            A[l + 1, slot(me_a), :] = h[0:blk]
            B[l + 1, slot(me_b), :] = h[blk : 2 * blk]
        with scope("drain"):
            for ref, s in [
                (A.at[l, pl.ds(0, rows - blk)], sa), (B.at[l, pl.ds(0, cols - blk)], sb),
                (cgot.at[l, pl.ds(0, 2 * nz - 1)], ssc), (rgot.at[l, pl.ds(0, nx * ny - 1)], ssr),
                (PR.at[l, pl.ds(0, nx * ny - 1), body], sp), (QX.at[l, :, body], sx),
                (QR.at[l, pl.ds(0, nz - 1), body], sq),
            ]:
                whole(ref, s, rq.at[l]).wait_send()
        return carry

    L = wq.shape[0]
    lax.fori_loop(0, L, layer, 0)
    with scope("exit"):
        last = [
            pltpu.make_async_copy(A.at[L, slot(me_a)], out.at[0], sl.at[0]),
            pltpu.make_async_copy(B.at[L, slot(me_b)], out.at[1], sl.at[1]),
        ]
        for c in last:
            c.start()
        for c in last:
            c.wait()


def align_all(dims, x, y, *weights):
    nx, ny, nz = dims
    ga, gb = nx * ny, nz * 2
    blk, d = x.shape
    rows, cols = ga * blk, gb * blk
    L = weights[0].shape[0]
    pad = blk + 8
    V, dma = pltpu.VMEM, lambda *s: pltpu.SemaphoreType.DMA(s)
    body = functools.partial(kernel, dims, blk * ga * gb)
    h = pl.pallas_call(
        body,
        out_shape=jax.ShapeDtypeStruct((2, blk, d), F32),
        in_specs=[pl.BlockSpec(memory_space=pl.ANY)] * 8,
        out_specs=pl.BlockSpec(memory_space=pl.ANY),
        scratch_shapes=[
            V((L + 1, rows, d), F32), V((L + 1, cols, d), F32), V((rows, cols), F32), V((cols // 256, rows, 256), F32),
            V((cols // 256, rows, 256), BF16), V((cols // 256, rows, 256), BF16),
            V((rows, 2 * d), BF16), V((rows, 2 * d), BF16),
            V((cols, 2 * d), BF16), V((cols, 2 * d), BF16), V((cols, 2 * d), BF16),
            V((d, rows), F32), V((2 * d + 16, rows), BF16), V((cols // 256, 256, 2 * d), BF16),
            V((rows, 128), F32), V((rows, 128), F32), V((rows, 128), F32),
            V((rows // 128, 128), F32), V((cols // 128, 128), F32),
            V((rows // 128, 128), F32), V((cols // 128, 128), F32),
            V((L, ga, rows // 128, 128), F32), V((L, gb, cols // 128, 128), F32),
            V((ga, pad, d), F32), V((L, ga, pad, d), F32),
            V((gb, pad, d), F32), V((L, nz, pad, d), F32), V((L, nz, pad, d), F32),
            *[V(w.shape, F32) for w in weights],
            V((2, 2 * d, weights[3].shape[2]), BF16), V((weights[3].shape[2], 2 * d), BF16),
            dma(8), dma(L), dma(L), dma(L), dma(L, nz), *[dma(L)] * 8, dma(L, cols // 256), dma(L), dma(L),
        ],
        compiler_params=pltpu.CompilerParams(
            collective_id=0, has_side_effects=True, vmem_limit_bytes=48 * 1024 * 1024
        ),
    )(*[pltpu.with_memory_space_constraint(a, pltpu.MemorySpace.HBM) for a in (x, y, *weights)])
    return h[0], h[1]


def solution(mesh):
    size = mesh.shape["row"] * mesh.shape["col"]
    dims = (4, 4, 8) if size == 256 else (2, 2, 2)
    placed = (P(("row", "col"), None), P(("row", "col"), None), P(), P(), P(), P(), P(), P())
    return jax.shard_map(
        functools.partial(align_all, dims),
        mesh=mesh,
        in_specs=placed,
        out_specs=(P(("row", "col"), None), P(("row", "col"), None)),
        check_vma=False,
    )
```

```python
import functools
import math

import jax
import jax.numpy as jnp
from jax import lax
from jax.experimental import pallas as pl
from jax.experimental.pallas import tpu as pltpu
from jax.sharding import PartitionSpec as P

MESH = pl.DeviceIdType.MESH
F32, BF16 = jnp.float32, jnp.bfloat16
HIGH = lax.Precision.HIGHEST
LOG2E = math.log2(math.e)
NT = (((1,), (1,)), ((), ()))


def dot(a, b, dims=(((1,), (0,)), ((), ()))):
    return lax.dot_general(a, b, dims, preferred_element_type=F32)


def high(a, b, dims=(((1,), (0,)), ((), ()))):
    return lax.dot_general(a, b, dims, precision=HIGH, preferred_element_type=F32)


def split2(v):
    top = v.astype(BF16)
    return top, (v - top.astype(F32)).astype(BF16)


def split3(v):
    top = v.astype(BF16)
    rest = v - top.astype(F32)
    mid = rest.astype(BF16)
    return top, mid, (rest - mid.astype(F32)).astype(BF16)


def eye(rows, shift=0):
    r = lax.broadcasted_iota(jnp.int32, (rows, 128), 0)
    c = lax.broadcasted_iota(jnp.int32, (rows, 128), 1)
    return c == r + shift


def to_lanes(column, mask):
    spread = jnp.broadcast_to(column, mask.shape)
    return jnp.sum(jnp.where(mask, spread, 0.0), axis=0, keepdims=True)


def to_rows(line, mask):
    spread = jnp.broadcast_to(line, mask.shape)
    return jnp.sum(jnp.where(mask, spread, 0.0), axis=1, keepdims=True)


def kernel(
    dims, total, x_ref, y_ref, wq_h, wk_h, gain_h, up_h, bias_h, down_h, out,
    A, B, S, E, MH, ML, T1, T2, K1, K2, K3, AF, AT, BC, RM, RS, RB, RW, CW,
    rsend, csend, rgot, cgot, PS, PR, QS, QX, QR,
    wq, wk, gain, up, bias, down, U, W,
    sl, sa, ra_, sb, rb_, rf, ssr, rsr, ssc, rsc, sp, rp, sx, rx, sq, rq,
):
    nx, ny, nz = dims
    row, col = lax.axis_index("row"), lax.axis_index("col")
    x, zl, k = lax.div(row, 4), lax.rem(lax.div(row, 2), 2), lax.rem(row, 2)
    zh, y = lax.div(col, ny), lax.rem(col, ny)
    z = zh * 2 + zl
    me_a, me_b = x * ny + y, z * 2 + k
    blk = x_ref.shape[0]
    rows, cols = nx * ny * blk, nz * 2 * blk
    cchunk, schunk = 256, min(256, rows)
    lanes = cchunk // 128
    offset = 0.05 / total
    factor = 2.0 / math.sqrt(x_ref.shape[1]) * LOG2E
    scope = jax.named_scope

    def at(x, y, z, k):
        return (x * 4 + lax.rem(z, 2) * 2 + k, lax.div(z, 2) * ny + y)

    def plane(n):
        px, py = lax.rem(x + n[0], nx), lax.rem(y + n[1], ny)
        return px * ny + py, at(px, py, z, k)

    def line(dz, other):
        pz = lax.rem(z + dz, nz)
        pk = 1 - k if other else k
        return pz * 2 + pk, at(x, y, pz, pk)

    near = lambda d, n: min(d, n - d)
    plane_steps = sorted(
        [(dx, dy) for dx in range(nx) for dy in range(ny) if (dx, dy) != (0, 0)],
        key=lambda s: -near(s[0], nx) - near(s[1], ny),
    )
    z_steps = sorted(range(1, nz), key=lambda d: near(d, nz))
    line_steps = [(d, o) for d in [*z_steps[::-1], 0] for o in (False, True) if (d, o) != (0, False)]
    _, sibling = line(0, True)

    def copy(src, dst, ss, rs, dev):
        return pltpu.make_async_remote_copy(
            src_ref=src, dst_ref=dst, send_sem=ss, recv_sem=rs, device_id=dev, device_id_type=MESH
        )

    def slot(n):
        return pl.ds(pl.multiple_of(n * blk, blk), blk)

    def chunk(n, size):
        return pl.ds(pl.multiple_of(n * size, size), size)

    with scope("entry"):
        barrier = pltpu.get_barrier_semaphore()
        for step in plane_steps:
            pl.semaphore_signal(barrier, inc=1, device_id=plane(step)[1], device_id_type=MESH)
        for step in line_steps:
            pl.semaphore_signal(barrier, inc=1, device_id=line(*step)[1], device_id_type=MESH)
        moves = [
            (x_ref, A.at[0, slot(me_a)]), (y_ref, B.at[0, slot(me_b)]), (wq_h, wq), (wk_h, wk),
            (gain_h, gain), (up_h, up), (bias_h, bias), (down_h, down),
        ]
        moves = [pltpu.make_async_copy(a, b, sl.at[n]) for n, (a, b) in enumerate(moves)]
        for m in moves:
            m.start()
        for m in moves[:2]:
            m.wait()
        pl.semaphore_wait(barrier, len(plane_steps) + len(line_steps))

    same, small = eye(128), eye(blk)

    def layer(l, carry):
        def send(src, dst, ss, rs, dev):
            copy(src, dst, ss.at[l], rs, dev).start()

        def whole(ref, ss, rs):
            return copy(ref, ref, ss.at[l], rs, sibling)

        own_a, own_b = A.at[l, slot(me_a)], B.at[l, slot(me_b)]
        send(own_b, own_b, sb, rf.at[l], sibling)
        for n, d in enumerate(z_steps[::-1]):
            send(own_b, own_b, sb, rb_.at[l, z], line(d, False)[1])
        for n, step in enumerate([(2, 2), (2, 0), (0, 2), (1, 1), (3, 3), (1, 2), (3, 2), (2, 1), (2, 3), (1, 3), (3, 1), (1, 0), (3, 0), (0, 1), (0, 3)]):
            send(own_a, own_a, sa, ra_.at[l], plane(step)[1])

        @pl.when(l == 0)
        def _():
            for m in moves[2:]:
                m.wait()

        m1, m2, m3 = split3(high(wk[l], wq[l], NT) * factor)
        stack = lambda a, b: jnp.concatenate([a, b], axis=0)
        mix_a = jnp.concatenate([stack(m1, m2), stack(m2, m1)], axis=1)
        mix_b = stack(m3, m1)

        def make_keys(at_):
            b1, b2, b3 = split3(B[l, at_, :])
            t = dot(jnp.concatenate([b1, b2], axis=1), mix_a)
            t = t[:, 0:128] + (t[:, 128:256] + dot(jnp.concatenate([b1, b3], axis=1), mix_b))
            k1, k2, k3 = split3(t)
            K1[at_, 0:128] = k1
            K1[at_, 128:256] = k2
            K2[at_, 0:128] = k2
            K2[at_, 128:256] = k1
            K3[at_, 0:128] = k3
            K3[at_, 128:256] = k1

        def make_rows(at_):
            a1, a2, a3 = split3(A[l, at_, :])
            T1[at_, 0:128] = a1
            T1[at_, 128:256] = a2
            T2[at_, 0:128] = a1
            T2[at_, 128:256] = a3

        with scope("gather"):
            for n, d in enumerate(z_steps[::-1]):
                s, _ = line(d, False)
                ref, pz = B.at[l, slot(s)], lax.rem(z + d, nz)
                whole(ref, sb, rb_.at[l, pz]).wait_recv()
                send(ref, ref, sb, rf.at[l], sibling)
                if n == 0:
                    make_keys(slot(me_b))
                if n < 2:
                    make_keys(slot(s))
            with scope("operands"):
                for d in z_steps[::-1][2:]:
                    make_keys(slot(line(d, False)[0]))
            whole(A.at[l, pl.ds(0, rows - blk)], sa, ra_.at[l]).wait_recv()
            with scope("operands"):
                for n in range(rows // 256):
                    make_rows(pl.ds(n * 256, 256))
            whole(B.at[l, pl.ds(0, cols // 2)], sb, rf.at[l]).wait_recv()
            with scope("operands"):
                for n in range(nz):
                    make_keys(slot(n * 2 + 1 - k))

        def product(n):
            at_ = pl.ds(n * schunk, schunk)
            t1, t2 = T1[at_, :], T2[at_, :]
            S[at_, :] = dot(t1, K1[...], NT) + dot(t1, K2[...], NT) + dot(t2, K3[...], NT)

        def row_statistics(n):
            for i in range(n * schunk, (n + 1) * schunk, 8):
                r = pl.ds(i, 8)
                parts = [S[r, j * 128 : (j + 1) * 128] for j in range(cols // 128)]
                m = functools.reduce(jnp.maximum, parts)
                RM[r, :] = m
                RS[r, :] = functools.reduce(jnp.add, [jnp.exp2(p - m) for p in parts])
            for i in range(n * schunk, (n + 1) * schunk, 128):
                at_ = pl.ds(i, 128)
                m = RM[at_, :]
                p = jnp.max(m, axis=1, keepdims=True)
                t = jnp.sum(RS[at_, :] * jnp.exp2(m - p), axis=1, keepdims=True)
                own = jnp.broadcast_to(p + jnp.log(t) * LOG2E, (128, 128))
                RB[at_, :] = own
                rsend[i // 128 : i // 128 + 1, :] = to_lanes(own, same)

        def column_statistics(j):
            at_ = pl.ds(j * cchunk, cchunk)
            m = [S[i * 8 : (i + 1) * 8, at_] for i in range(4)]
            for i in range(32, rows, 32):
                m = [jnp.maximum(m[e], S[i + e * 8 : i + e * 8 + 8, at_]) for e in range(4)]
            p = jnp.max(functools.reduce(jnp.maximum, m), axis=0, keepdims=True)
            pb = jnp.broadcast_to(p, (8, cchunk))
            t = [jnp.zeros((8, cchunk), F32)] * 4
            for i in range(0, rows, 32):
                t = [t[e] + jnp.exp2(S[i + e * 8 : i + e * 8 + 8, at_] - pb) for e in range(4)]
            c = p + jnp.log(jnp.sum(functools.reduce(jnp.add, t), axis=0, keepdims=True)) * LOG2E
            for e in range(lanes):
                csend[j * lanes + e : j * lanes + e + 1, :] = c[:, e * 128 : (e + 1) * 128]

        with scope("score"):
            product(0)
            for n in range(rows // schunk):
                if n + 1 < rows // schunk:
                    product(n + 1)
                row_statistics(n)
            for n, step in enumerate(plane_steps):
                send(rsend, rgot.at[l, me_a], ssr, rsr.at[l], plane(step)[1])
        with scope("lse"):
            for j in range(cols // cchunk):
                column_statistics(j)
            for n, step in enumerate(line_steps):
                send(csend, cgot.at[l, me_b], ssc, rsc.at[l], line(*step)[1])
        cgot[l, me_b] = csend[...]
        rgot[l, me_a] = rsend[...]
        turns = {4: (2, 1, 3, 0), 2: (1, 0), 1: (0,)}
        cturn = turns[cols // cchunk]
        parcels = {
            4: [
                [(2, 2), (2, 0), (0, 2), (1, 1)], [(1, 2), (3, 2), (2, 1), (2, 3)],
                [(1, 3), (3, 1), (3, 3), (1, 0)], [(3, 0), (0, 1), (0, 3), (0, 0)],
            ],
            2: [[(1, 1), (1, 0), (0, 1), (0, 0)]],
        }[nx]
        body = pl.ds(0, blk + 1)

        def column_line(ref, b):
            return jnp.concatenate([ref[pl.ds(b * lanes + j, 1), :] for j in range(lanes)], axis=1)

        def matches(n):
            b = lax.rem(zh + cturn[n], len(cturn))
            at_ = chunk(b, cchunk)
            cb = jnp.broadcast_to(column_line(csend, b), (16, cchunk))
            for i in range(0, rows, 16):
                r = pl.ds(i, 16)
                s = S[r, at_]
                rb = RB[r, :]
                m = jnp.exp2((s - jnp.concatenate([rb] * lanes, axis=1)) + (s - cb))
                E[n, r, :] = m
                h, lo = split2(m)
                MH[n, r, :] = h
                ML[n, r, :] = lo

        with scope("match"):
            for n in range(rows // 128):
                AF[:, n * 128 : (n + 1) * 128] = A[l, n * 128 : (n + 1) * 128, :].T
            for n in range(len(cturn)):
                matches(n)

        def lse(got):
            p = jnp.max(got, axis=0)
            return p + jnp.log(jnp.sum(jnp.exp2(got - p), axis=0)) * LOG2E

        with scope("weights"):
            u1, u2 = split2(up[l])
            U[0, 0:128, :] = u1
            U[0, 128:256, :] = u1
            U[1, 0:128, :] = u2
            U[1, 128:256, :] = u2
            w1, w2 = split2(down[l])
            W[:, 0:128] = w1
            W[:, 128:256] = w2
        with scope("wait_rows"):
            whole(rgot.at[l, pl.ds(0, nx * ny - 1)], ssr, rsr.at[l]).wait_recv()
        if True:
            RW[...] = jnp.exp2(rsend[...] - lse(rgot[l]))
            first = lax.broadcasted_iota(jnp.int32, (16, 128), 0)
            for n in range(rows // 128):
                cut = pl.ds(n * 128, 128)
                v = RW[n : n + 1, :]
                t1, t2 = split2(AF[:, cut] * v)
                AT[0:128, cut] = t2
                AT[128:256, cut] = t1
                low = v - v.astype(BF16).astype(F32)
                AT[256:272, cut] = jnp.where(
                    first == 0, v, jnp.where(first == 1, low, 0.0)
                ).astype(BF16)
                RB[cut, :] = jnp.broadcast_to(to_rows(v, same), (128, 128))

        def column_weights():
            with scope("wait_columns"):
                whole(cgot.at[l, pl.ds(0, 2 * nz - 1)], ssc, rsc.at[l]).wait_recv()
            CW[...] = jnp.exp2(csend[...] - lse(cgot[l]))

        def first_operands():
            with scope("spread"):
                for n, turn in enumerate(cturn):
                    b = lax.rem(zh + turn, len(cturn))
                    for j in range(lanes):
                        w = to_rows(CW[pl.ds(b * lanes + j, 1), :], same)
                        b1, b2 = split2(B[l, chunk(b * lanes + j, 128), :] * w)
                        BC[n, j * 128 : (j + 1) * 128, 0:128] = b1
                        BC[n, j * 128 : (j + 1) * 128, 128:256] = b2

        def to_second(n):
            q = dot(AT[...], MH[n])
            u = dot(AT[128:272, :], ML[n])
            if n == 0:
                column_weights()
            b = lax.rem(zh + cturn[n], len(cturn))
            w = column_line(CW, b)
            mass = (q[256:257] + q[257:258] + u[128:129] + u[129:130]) * w
            q = (q[0:128] + q[128:256] + u[0:128]) * w
            for j in range(lanes):
                t = q[:, j * 128 : (j + 1) * 128].T
                for e in range(2):
                    QS[(b * lanes + j) * 2 + e, 0:blk, :] = t[e * blk : (e + 1) * blk]
                    QS[(b * lanes + j) * 2 + e, blk : blk + 1, :] = mass[:, j * 128 : (j + 1) * 128]

        def turned(n):
            return lax.rem(zh + cturn[n], len(cturn))

        def cross(n):
            for j in range(lanes):
                pz = turned(n) * lanes + j
                send(QS.at[pz * 2 + (1 - k), body], QX.at[l, pz, body], sx, rx.at[l, turned(n)], sibling)

        def join(n):
            b = turned(n)
            whole(QX.at[l, pl.ds(b * lanes, lanes), body], sx, rx.at[l, b]).wait_recv()
            for pz in [b * lanes, b * lanes + 1] if cturn[n] else [b * lanes + 1 - zl]:
                QS[pz * 2 + k, body] = QS[pz * 2 + k, body] + QX[l, pz, body]
                send(QS.at[pz * 2 + k, body], QR.at[l, z, body], sq, rq.at[l], at(x, y, pz, k))
            if not cturn[n]:
                QR[l, z, body] = QS[z * 2 + k, body] + QX[l, z, body]

        def to_first(n):
            owners = [plane(o)[0] for o in parcels[n]]
            left = lambda ref: jnp.concatenate([ref[slot(s), :] for s in owners], axis=0)
            p = sum(dot(left(MH.at[j]), BC[j]) for j in range(len(cturn)))
            p = p[:, 0:128] + p[:, 128:256]
            p = p + sum(dot(left(ML.at[j]), BC[j, :, 0:128]) for j in range(len(cturn)))
            for e, s in enumerate(owners):
                parts = []
                for j, turn in enumerate(cturn):
                    w = column_line(CW, lax.rem(zh + turn, len(cturn)))
                    t = E[j, slot(s), :] * w
                    parts += [t[:, m * 128 : (m + 1) * 128] for m in range(lanes)]
                v = RB[slot(s), :]
                mass = jnp.sum(functools.reduce(jnp.add, parts) * v, axis=1, keepdims=True)
                PS[s, 0:blk, :] = p[e * blk : (e + 1) * blk] * v
                PS[s, blk : blk + 1, :] = to_lanes(mass, small)

        def give(n):
            to_first(n)
            for o in parcels[n]:
                s, dev = plane(o)
                if o != (0, 0):
                    send(PS.at[s, body], PR.at[l, me_a, body], sp, rp.at[l], dev)
                else:
                    PR[l, me_a, body] = PS[me_a, body]

        with scope("messages"):
            def second(n):
                with scope("second"):
                    to_second(n)
                cross(n)
                if n == 0:
                    first_operands()

            def first(n):
                with scope("first"):
                    give(n)

            def joined(n):
                with scope("join"):
                    join(n)

            if len(cturn) == 4:
                for f, n in zip(
                    (second, first, joined, second, first, second, joined, first, joined, second, first, joined),
                    (0, 0, 0, 1, 1, 2, 1, 2, 2, 3, 3, 3),
                ):
                    f(n)
            else:
                for n in range(len(cturn)):
                    second(n)
                    joined(n)
                for n in range(len(parcels)):
                    first(n)

        with scope("wait_q"):
            whole(QR.at[l, pl.ds(0, nz - 1), body], sq, rq.at[l]).wait_recv()
        q = jnp.sum(QR[l, :, body], axis=0)
        qm = to_rows(q[blk : blk + 1], eye(blk, lax.rem(me_b, 2) * blk))
        hy = B[l, slot(me_b), :] + q[0:blk] / (qm + offset)
        with scope("wait_p"):
            whole(PR.at[l, pl.ds(0, nx * ny - 1), body], sp, rp.at[l]).wait_recv()
        with scope("refine"):
            p = jnp.sum(PR[l, :, body], axis=0)
            pm = to_rows(p[blk : blk + 1], small)
            hx = A[l, slot(me_a), :] + p[0:blk] / (pm + offset)
            h = jnp.concatenate([hx, hy], axis=0)
            scale = lax.rsqrt(jnp.mean(h * h, axis=1, keepdims=True) + 1e-05)
            n1, n2 = split2(h * scale * gain[pl.ds(l, 1), :])
            n12 = jnp.concatenate([n1, n2], axis=1)
            u = dot(n12, U[0]) + dot(n12, U[1]) + bias[pl.ds(l, 1), :]
            g = 0.5 * u * (1.0 + jnp.tanh(math.sqrt(2 / math.pi) * (u + 0.044715 * (u * u * u))))
            g1, g2 = split2(g)
            t = dot(g1, W[...]) + dot(g2, W[...])
            h = h + (t[:, 0:128] + t[:, 128:256])
            A[l + 1, slot(me_a), :] = h[0:blk]
            B[l + 1, slot(me_b), :] = h[blk : 2 * blk]
        with scope("drain"):
            for ref, s in [
                (A.at[l, pl.ds(0, rows - blk)], sa), (B.at[l, pl.ds(0, cols - blk)], sb),
                (cgot.at[l, pl.ds(0, 2 * nz - 1)], ssc), (rgot.at[l, pl.ds(0, nx * ny - 1)], ssr),
                (PR.at[l, pl.ds(0, nx * ny - 1), body], sp), (QX.at[l, :, body], sx),
                (QR.at[l, pl.ds(0, nz - 1), body], sq),
            ]:
                whole(ref, s, rq.at[l]).wait_send()
        return carry

    L = wq.shape[0]
    lax.fori_loop(0, L, layer, 0)
    with scope("exit"):
        last = [
            pltpu.make_async_copy(A.at[L, slot(me_a)], out.at[0], sl.at[0]),
            pltpu.make_async_copy(B.at[L, slot(me_b)], out.at[1], sl.at[1]),
        ]
        for c in last:
            c.start()
        for c in last:
            c.wait()


def align_all(dims, x, y, *weights):
    nx, ny, nz = dims
    ga, gb = nx * ny, nz * 2
    blk, d = x.shape
    rows, cols = ga * blk, gb * blk
    L = weights[0].shape[0]
    pad = blk + 8
    V, dma = pltpu.VMEM, lambda *s: pltpu.SemaphoreType.DMA(s)
    body = functools.partial(kernel, dims, blk * ga * gb)
    h = pl.pallas_call(
        body,
        out_shape=jax.ShapeDtypeStruct((2, blk, d), F32),
        in_specs=[pl.BlockSpec(memory_space=pl.ANY)] * 8,
        out_specs=pl.BlockSpec(memory_space=pl.ANY),
        scratch_shapes=[
            V((L + 1, rows, d), F32), V((L + 1, cols, d), F32), V((rows, cols), F32), V((cols // 256, rows, 256), F32),
            V((cols // 256, rows, 256), BF16), V((cols // 256, rows, 256), BF16),
            V((rows, 2 * d), BF16), V((rows, 2 * d), BF16),
            V((cols, 2 * d), BF16), V((cols, 2 * d), BF16), V((cols, 2 * d), BF16),
            V((d, rows), F32), V((2 * d + 16, rows), BF16), V((cols // 256, 256, 2 * d), BF16),
            V((rows, 128), F32), V((rows, 128), F32), V((rows, 128), F32),
            V((rows // 128, 128), F32), V((cols // 128, 128), F32),
            V((rows // 128, 128), F32), V((cols // 128, 128), F32),
            V((L, ga, rows // 128, 128), F32), V((L, gb, cols // 128, 128), F32),
            V((ga, pad, d), F32), V((L, ga, pad, d), F32),
            V((gb, pad, d), F32), V((L, nz, pad, d), F32), V((L, nz, pad, d), F32),
            *[V(w.shape, F32) for w in weights],
            V((2, 2 * d, weights[3].shape[2]), BF16), V((weights[3].shape[2], 2 * d), BF16),
            dma(8), dma(L), dma(L), dma(L), dma(L, nz), *[dma(L)] * 8, dma(L, cols // 256), dma(L), dma(L),
        ],
        compiler_params=pltpu.CompilerParams(
            collective_id=0, has_side_effects=True, vmem_limit_bytes=48 * 1024 * 1024
        ),
    )(*[pltpu.with_memory_space_constraint(a, pltpu.MemorySpace.HBM) for a in (x, y, *weights)])
    return h[0], h[1]


def solution(mesh):
    size = mesh.shape["row"] * mesh.shape["col"]
    dims = (4, 4, 8) if size == 256 else (2, 2, 2)
    placed = (P(("row", "col"), None), P(("row", "col"), None), P(), P(), P(), P(), P(), P())
    return jax.shard_map(
        functools.partial(align_all, dims),
        mesh=mesh,
        in_specs=placed,
        out_specs=(P(("row", "col"), None), P(("row", "col"), None)),
        check_vma=False,
    )
```

```python
import functools
import math

import jax
import jax.numpy as jnp
from jax import lax
from jax.experimental import pallas as pl
from jax.experimental.pallas import tpu as pltpu
from jax.sharding import PartitionSpec as P

MESH = pl.DeviceIdType.MESH
F32, BF16 = jnp.float32, jnp.bfloat16
HIGH = lax.Precision.HIGHEST
LOG2E = math.log2(math.e)
NT = (((1,), (1,)), ((), ()))


def dot(a, b, dims=(((1,), (0,)), ((), ()))):
    return lax.dot_general(a, b, dims, preferred_element_type=F32)


def high(a, b, dims=(((1,), (0,)), ((), ()))):
    return lax.dot_general(a, b, dims, precision=HIGH, preferred_element_type=F32)


def split2(v):
    top = v.astype(BF16)
    return top, (v - top.astype(F32)).astype(BF16)


def split3(v):
    top = v.astype(BF16)
    rest = v - top.astype(F32)
    mid = rest.astype(BF16)
    return top, mid, (rest - mid.astype(F32)).astype(BF16)


def eye(rows, shift=0):
    r = lax.broadcasted_iota(jnp.int32, (rows, 128), 0)
    c = lax.broadcasted_iota(jnp.int32, (rows, 128), 1)
    return c == r + shift


def to_lanes(column, mask):
    spread = jnp.broadcast_to(column, mask.shape)
    return jnp.sum(jnp.where(mask, spread, 0.0), axis=0, keepdims=True)


def to_rows(line, mask):
    spread = jnp.broadcast_to(line, mask.shape)
    return jnp.sum(jnp.where(mask, spread, 0.0), axis=1, keepdims=True)


def kernel(
    dims, total, x_ref, y_ref, wq_h, wk_h, gain_h, up_h, bias_h, down_h, out,
    A, B, S, E, MH, ML, T1, T2, K1, K2, K3, AF, AT, BC, RM, RS, RB, RW, CW,
    rsend, csend, rgot, cgot, PS, PR, QS, QX, QR,
    wq, wk, gain, up, bias, down, U, W,
    sl, sa, ra_, sb, rb_, rf, ssr, rsr, ssc, rsc, sp, rp, sx, rx, sq, rq,
):
    nx, ny, nz = dims
    row, col = lax.axis_index("row"), lax.axis_index("col")
    x, zl, k = lax.div(row, 4), lax.rem(lax.div(row, 2), 2), lax.rem(row, 2)
    zh, y = lax.div(col, ny), lax.rem(col, ny)
    z = zh * 2 + zl
    me_a, me_b = x * ny + y, z * 2 + k
    blk = x_ref.shape[0]
    rows, cols = nx * ny * blk, nz * 2 * blk
    cchunk, schunk = 256, min(256, rows)
    lanes = cchunk // 128
    offset = 0.05 / total
    factor = 2.0 / math.sqrt(x_ref.shape[1]) * LOG2E
    scope = jax.named_scope

    def at(x, y, z, k):
        return (x * 4 + lax.rem(z, 2) * 2 + k, lax.div(z, 2) * ny + y)

    def plane(n):
        px, py = lax.rem(x + n[0], nx), lax.rem(y + n[1], ny)
        return px * ny + py, at(px, py, z, k)

    def line(dz, other):
        pz = lax.rem(z + dz, nz)
        pk = 1 - k if other else k
        return pz * 2 + pk, at(x, y, pz, pk)

    near = lambda d, n: min(d, n - d)
    plane_steps = sorted(
        [(dx, dy) for dx in range(nx) for dy in range(ny) if (dx, dy) != (0, 0)],
        key=lambda s: -near(s[0], nx) - near(s[1], ny),
    )
    z_steps = sorted(range(1, nz), key=lambda d: near(d, nz))
    line_steps = [(d, o) for d in [*z_steps[::-1], 0] for o in (False, True) if (d, o) != (0, False)]
    _, sibling = line(0, True)

    def copy(src, dst, ss, rs, dev):
        return pltpu.make_async_remote_copy(
            src_ref=src, dst_ref=dst, send_sem=ss, recv_sem=rs, device_id=dev, device_id_type=MESH
        )

    def slot(n):
        return pl.ds(pl.multiple_of(n * blk, blk), blk)

    def chunk(n, size):
        return pl.ds(pl.multiple_of(n * size, size), size)

    with scope("entry"):
        barrier = pltpu.get_barrier_semaphore()
        for step in plane_steps:
            pl.semaphore_signal(barrier, inc=1, device_id=plane(step)[1], device_id_type=MESH)
        for step in line_steps:
            pl.semaphore_signal(barrier, inc=1, device_id=line(*step)[1], device_id_type=MESH)
        moves = [
            (x_ref, A.at[0, slot(me_a)]), (y_ref, B.at[0, slot(me_b)]), (wq_h, wq), (wk_h, wk),
            (gain_h, gain), (up_h, up), (bias_h, bias), (down_h, down),
        ]
        moves = [pltpu.make_async_copy(a, b, sl.at[n]) for n, (a, b) in enumerate(moves)]
        for m in moves:
            m.start()
        for m in moves[:2]:
            m.wait()
        pl.semaphore_wait(barrier, len(plane_steps) + len(line_steps))

    same, small = eye(128), eye(blk)

    def layer(l, carry):
        def send(src, dst, ss, rs, dev):
            copy(src, dst, ss.at[l], rs, dev).start()

        def whole(ref, ss, rs):
            return copy(ref, ref, ss.at[l], rs, sibling)

        own_a, own_b = A.at[l, slot(me_a)], B.at[l, slot(me_b)]
        send(own_b, own_b, sb, rf.at[l], sibling)
        for n, d in enumerate(z_steps[::-1]):
            send(own_b, own_b, sb, rb_.at[l, z], line(d, False)[1])
            if d in (1, nz - 1):
                send(own_b, own_b, sb, rf.at[l], line(d, True)[1])
        for n, step in enumerate([(2, 2), (2, 0), (0, 2), (1, 1), (3, 3), (1, 2), (3, 2), (2, 1), (2, 3), (1, 3), (3, 1), (1, 0), (3, 0), (0, 1), (0, 3)]):
            send(own_a, own_a, sa, ra_.at[l], plane(step)[1])

        @pl.when(l == 0)
        def _():
            for m in moves[2:]:
                m.wait()

        m1, m2, m3 = split3(high(wk[l], wq[l], NT) * factor)
        stack = lambda a, b: jnp.concatenate([a, b], axis=0)
        mix_a = jnp.concatenate([stack(m1, m2), stack(m2, m1)], axis=1)
        mix_b = stack(m3, m1)

        def make_keys(at_):
            b1, b2, b3 = split3(B[l, at_, :])
            t = dot(jnp.concatenate([b1, b2], axis=1), mix_a)
            t = t[:, 0:128] + (t[:, 128:256] + dot(jnp.concatenate([b1, b3], axis=1), mix_b))
            k1, k2, k3 = split3(t)
            K1[at_, 0:128] = k1
            K1[at_, 128:256] = k2
            K2[at_, 0:128] = k2
            K2[at_, 128:256] = k1
            K3[at_, 0:128] = k3
            K3[at_, 128:256] = k1

        def make_rows(at_):
            a1, a2, a3 = split3(A[l, at_, :])
            T1[at_, 0:128] = a1
            T1[at_, 128:256] = a2
            T2[at_, 0:128] = a1
            T2[at_, 128:256] = a3

        with scope("gather"):
            for n, d in enumerate(z_steps[::-1]):
                s, _ = line(d, False)
                ref, pz = B.at[l, slot(s)], lax.rem(z + d, nz)
                whole(ref, sb, rb_.at[l, pz]).wait_recv()
                if d not in (1, nz - 1):
                    send(ref, ref, sb, rf.at[l], sibling)
                if n == 0:
                    make_keys(slot(me_b))
                if n < 2:
                    make_keys(slot(s))
            with scope("operands"):
                for d in z_steps[::-1][2:]:
                    make_keys(slot(line(d, False)[0]))
            whole(A.at[l, pl.ds(0, rows - blk)], sa, ra_.at[l]).wait_recv()
            with scope("operands"):
                for n in range(rows // 256):
                    make_rows(pl.ds(n * 256, 256))
            whole(B.at[l, pl.ds(0, cols // 2)], sb, rf.at[l]).wait_recv()
            with scope("operands"):
                for n in range(nz):
                    make_keys(slot(n * 2 + 1 - k))

        def product(n):
            at_ = pl.ds(n * schunk, schunk)
            t1, t2 = T1[at_, :], T2[at_, :]
            S[at_, :] = dot(t1, K1[...], NT) + dot(t1, K2[...], NT) + dot(t2, K3[...], NT)

        def row_statistics(n):
            for i in range(n * schunk, (n + 1) * schunk, 8):
                r = pl.ds(i, 8)
                parts = [S[r, j * 128 : (j + 1) * 128] for j in range(cols // 128)]
                m = functools.reduce(jnp.maximum, parts)
                RM[r, :] = m
                RS[r, :] = functools.reduce(jnp.add, [jnp.exp2(p - m) for p in parts])
            for i in range(n * schunk, (n + 1) * schunk, 128):
                at_ = pl.ds(i, 128)
                m = RM[at_, :]
                p = jnp.max(m, axis=1, keepdims=True)
                t = jnp.sum(RS[at_, :] * jnp.exp2(m - p), axis=1, keepdims=True)
                own = jnp.broadcast_to(p + jnp.log(t) * LOG2E, (128, 128))
                RB[at_, :] = own
                rsend[i // 128 : i // 128 + 1, :] = to_lanes(own, same)

        def column_statistics(j):
            at_ = pl.ds(j * cchunk, cchunk)
            m = [S[i * 8 : (i + 1) * 8, at_] for i in range(4)]
            for i in range(32, rows, 32):
                m = [jnp.maximum(m[e], S[i + e * 8 : i + e * 8 + 8, at_]) for e in range(4)]
            p = jnp.max(functools.reduce(jnp.maximum, m), axis=0, keepdims=True)
            pb = jnp.broadcast_to(p, (8, cchunk))
            t = [jnp.zeros((8, cchunk), F32)] * 4
            for i in range(0, rows, 32):
                t = [t[e] + jnp.exp2(S[i + e * 8 : i + e * 8 + 8, at_] - pb) for e in range(4)]
            c = p + jnp.log(jnp.sum(functools.reduce(jnp.add, t), axis=0, keepdims=True)) * LOG2E
            for e in range(lanes):
                csend[j * lanes + e : j * lanes + e + 1, :] = c[:, e * 128 : (e + 1) * 128]

        with scope("score"):
            product(0)
            for n in range(rows // schunk):
                if n + 1 < rows // schunk:
                    product(n + 1)
                row_statistics(n)
            for n, step in enumerate(plane_steps):
                send(rsend, rgot.at[l, me_a], ssr, rsr.at[l], plane(step)[1])
        with scope("lse"):
            for j in range(cols // cchunk):
                column_statistics(j)
            for n, step in enumerate(line_steps):
                send(csend, cgot.at[l, me_b], ssc, rsc.at[l], line(*step)[1])
        cgot[l, me_b] = csend[...]
        rgot[l, me_a] = rsend[...]
        turns = {4: (2, 1, 3, 0), 2: (1, 0), 1: (0,)}
        cturn = turns[cols // cchunk]
        parcels = {
            4: [
                [(2, 2), (2, 0), (0, 2), (1, 1)], [(1, 2), (3, 2), (2, 1), (2, 3)],
                [(1, 3), (3, 1), (3, 3), (1, 0)], [(3, 0), (0, 1), (0, 3), (0, 0)],
            ],
            2: [[(1, 1), (1, 0), (0, 1), (0, 0)]],
        }[nx]
        body = pl.ds(0, blk + 1)

        def column_line(ref, b):
            return jnp.concatenate([ref[pl.ds(b * lanes + j, 1), :] for j in range(lanes)], axis=1)

        def matches(n):
            b = lax.rem(zh + cturn[n], len(cturn))
            at_ = chunk(b, cchunk)
            cb = jnp.broadcast_to(column_line(csend, b), (16, cchunk))
            for i in range(0, rows, 16):
                r = pl.ds(i, 16)
                s = S[r, at_]
                rb = RB[r, :]
                m = jnp.exp2((s - jnp.concatenate([rb] * lanes, axis=1)) + (s - cb))
                E[n, r, :] = m
                h, lo = split2(m)
                MH[n, r, :] = h
                ML[n, r, :] = lo

        with scope("match"):
            for n in range(rows // 128):
                AF[:, n * 128 : (n + 1) * 128] = A[l, n * 128 : (n + 1) * 128, :].T
            for n in range(len(cturn)):
                matches(n)

        def lse(got):
            p = jnp.max(got, axis=0)
            return p + jnp.log(jnp.sum(jnp.exp2(got - p), axis=0)) * LOG2E

        with scope("weights"):
            u1, u2 = split2(up[l])
            U[0, 0:128, :] = u1
            U[0, 128:256, :] = u1
            U[1, 0:128, :] = u2
            U[1, 128:256, :] = u2
            w1, w2 = split2(down[l])
            W[:, 0:128] = w1
            W[:, 128:256] = w2
        with scope("wait_rows"):
            whole(rgot.at[l, pl.ds(0, nx * ny - 1)], ssr, rsr.at[l]).wait_recv()
        if True:
            RW[...] = jnp.exp2(rsend[...] - lse(rgot[l]))
            first = lax.broadcasted_iota(jnp.int32, (16, 128), 0)
            for n in range(rows // 128):
                cut = pl.ds(n * 128, 128)
                v = RW[n : n + 1, :]
                t1, t2 = split2(AF[:, cut] * v)
                AT[0:128, cut] = t2
                AT[128:256, cut] = t1
                low = v - v.astype(BF16).astype(F32)
                AT[256:272, cut] = jnp.where(
                    first == 0, v, jnp.where(first == 1, low, 0.0)
                ).astype(BF16)
                RB[cut, :] = jnp.broadcast_to(to_rows(v, same), (128, 128))

        def column_weights():
            with scope("wait_columns"):
                whole(cgot.at[l, pl.ds(0, 2 * nz - 1)], ssc, rsc.at[l]).wait_recv()
            CW[...] = jnp.exp2(csend[...] - lse(cgot[l]))

        def first_operands():
            with scope("spread"):
                for n, turn in enumerate(cturn):
                    b = lax.rem(zh + turn, len(cturn))
                    for j in range(lanes):
                        w = to_rows(CW[pl.ds(b * lanes + j, 1), :], same)
                        b1, b2 = split2(B[l, chunk(b * lanes + j, 128), :] * w)
                        BC[n, j * 128 : (j + 1) * 128, 0:128] = b1
                        BC[n, j * 128 : (j + 1) * 128, 128:256] = b2

        def to_second(n):
            q = dot(AT[...], MH[n])
            u = dot(AT[128:272, :], ML[n])
            if n == 0:
                column_weights()
            b = lax.rem(zh + cturn[n], len(cturn))
            w = column_line(CW, b)
            mass = (q[256:257] + q[257:258] + u[128:129] + u[129:130]) * w
            q = (q[0:128] + q[128:256] + u[0:128]) * w
            for j in range(lanes):
                t = q[:, j * 128 : (j + 1) * 128].T
                for e in range(2):
                    QS[(b * lanes + j) * 2 + e, 0:blk, :] = t[e * blk : (e + 1) * blk]
                    QS[(b * lanes + j) * 2 + e, blk : blk + 1, :] = mass[:, j * 128 : (j + 1) * 128]

        def turned(n):
            return lax.rem(zh + cturn[n], len(cturn))

        def cross(n):
            for j in range(lanes):
                pz = turned(n) * lanes + j
                send(QS.at[pz * 2 + (1 - k), body], QX.at[l, pz, body], sx, rx.at[l, turned(n)], sibling)

        def join(n):
            b = turned(n)
            whole(QX.at[l, pl.ds(b * lanes, lanes), body], sx, rx.at[l, b]).wait_recv()
            for pz in [b * lanes, b * lanes + 1] if cturn[n] else [b * lanes + 1 - zl]:
                QS[pz * 2 + k, body] = QS[pz * 2 + k, body] + QX[l, pz, body]
                send(QS.at[pz * 2 + k, body], QR.at[l, z, body], sq, rq.at[l], at(x, y, pz, k))
            if not cturn[n]:
                QR[l, z, body] = QS[z * 2 + k, body] + QX[l, z, body]

        def to_first(n):
            owners = [plane(o)[0] for o in parcels[n]]
            left = lambda ref: jnp.concatenate([ref[slot(s), :] for s in owners], axis=0)
            p = sum(dot(left(MH.at[j]), BC[j]) for j in range(len(cturn)))
            p = p[:, 0:128] + p[:, 128:256]
            p = p + sum(dot(left(ML.at[j]), BC[j, :, 0:128]) for j in range(len(cturn)))
            for e, s in enumerate(owners):
                parts = []
                for j, turn in enumerate(cturn):
                    w = column_line(CW, lax.rem(zh + turn, len(cturn)))
                    t = E[j, slot(s), :] * w
                    parts += [t[:, m * 128 : (m + 1) * 128] for m in range(lanes)]
                v = RB[slot(s), :]
                mass = jnp.sum(functools.reduce(jnp.add, parts) * v, axis=1, keepdims=True)
                PS[s, 0:blk, :] = p[e * blk : (e + 1) * blk] * v
                PS[s, blk : blk + 1, :] = to_lanes(mass, small)

        def give(n):
            to_first(n)
            for o in parcels[n]:
                s, dev = plane(o)
                if o != (0, 0):
                    send(PS.at[s, body], PR.at[l, me_a, body], sp, rp.at[l], dev)
                else:
                    PR[l, me_a, body] = PS[me_a, body]

        with scope("messages"):
            def second(n):
                with scope("second"):
                    to_second(n)
                cross(n)
                if n == 0:
                    first_operands()

            def first(n):
                with scope("first"):
                    give(n)

            def joined(n):
                with scope("join"):
                    join(n)

            if len(cturn) == 4:
                for f, n in zip(
                    (second, first, joined, second, first, second, joined, first, joined, second, first, joined),
                    (0, 0, 0, 1, 1, 2, 1, 2, 2, 3, 3, 3),
                ):
                    f(n)
            else:
                for n in range(len(cturn)):
                    second(n)
                    joined(n)
                for n in range(len(parcels)):
                    first(n)

        with scope("wait_q"):
            whole(QR.at[l, pl.ds(0, nz - 1), body], sq, rq.at[l]).wait_recv()
        q = jnp.sum(QR[l, :, body], axis=0)
        qm = to_rows(q[blk : blk + 1], eye(blk, lax.rem(me_b, 2) * blk))
        hy = B[l, slot(me_b), :] + q[0:blk] / (qm + offset)
        with scope("wait_p"):
            whole(PR.at[l, pl.ds(0, nx * ny - 1), body], sp, rp.at[l]).wait_recv()
        with scope("refine"):
            p = jnp.sum(PR[l, :, body], axis=0)
            pm = to_rows(p[blk : blk + 1], small)
            hx = A[l, slot(me_a), :] + p[0:blk] / (pm + offset)
            h = jnp.concatenate([hx, hy], axis=0)
            scale = lax.rsqrt(jnp.mean(h * h, axis=1, keepdims=True) + 1e-05)
            n1, n2 = split2(h * scale * gain[pl.ds(l, 1), :])
            n12 = jnp.concatenate([n1, n2], axis=1)
            u = dot(n12, U[0]) + dot(n12, U[1]) + bias[pl.ds(l, 1), :]
            g = 0.5 * u * (1.0 + jnp.tanh(math.sqrt(2 / math.pi) * (u + 0.044715 * (u * u * u))))
            g1, g2 = split2(g)
            t = dot(g1, W[...]) + dot(g2, W[...])
            h = h + (t[:, 0:128] + t[:, 128:256])
            A[l + 1, slot(me_a), :] = h[0:blk]
            B[l + 1, slot(me_b), :] = h[blk : 2 * blk]
        with scope("drain"):
            for ref, s in [
                (A.at[l, pl.ds(0, rows - blk)], sa), (B.at[l, pl.ds(0, cols - blk)], sb),
                (cgot.at[l, pl.ds(0, 2 * nz - 1)], ssc), (rgot.at[l, pl.ds(0, nx * ny - 1)], ssr),
                (PR.at[l, pl.ds(0, nx * ny - 1), body], sp), (QX.at[l, :, body], sx),
                (QR.at[l, pl.ds(0, nz - 1), body], sq),
            ]:
                whole(ref, s, rq.at[l]).wait_send()
        return carry

    L = wq.shape[0]
    lax.fori_loop(0, L, layer, 0)
    with scope("exit"):
        last = [
            pltpu.make_async_copy(A.at[L, slot(me_a)], out.at[0], sl.at[0]),
            pltpu.make_async_copy(B.at[L, slot(me_b)], out.at[1], sl.at[1]),
        ]
        for c in last:
            c.start()
        for c in last:
            c.wait()


def align_all(dims, x, y, *weights):
    nx, ny, nz = dims
    ga, gb = nx * ny, nz * 2
    blk, d = x.shape
    rows, cols = ga * blk, gb * blk
    L = weights[0].shape[0]
    pad = blk + 8
    V, dma = pltpu.VMEM, lambda *s: pltpu.SemaphoreType.DMA(s)
    body = functools.partial(kernel, dims, blk * ga * gb)
    h = pl.pallas_call(
        body,
        out_shape=jax.ShapeDtypeStruct((2, blk, d), F32),
        in_specs=[pl.BlockSpec(memory_space=pl.ANY)] * 8,
        out_specs=pl.BlockSpec(memory_space=pl.ANY),
        scratch_shapes=[
            V((L + 1, rows, d), F32), V((L + 1, cols, d), F32), V((rows, cols), F32), V((cols // 256, rows, 256), F32),
            V((cols // 256, rows, 256), BF16), V((cols // 256, rows, 256), BF16),
            V((rows, 2 * d), BF16), V((rows, 2 * d), BF16),
            V((cols, 2 * d), BF16), V((cols, 2 * d), BF16), V((cols, 2 * d), BF16),
            V((d, rows), F32), V((2 * d + 16, rows), BF16), V((cols // 256, 256, 2 * d), BF16),
            V((rows, 128), F32), V((rows, 128), F32), V((rows, 128), F32),
            V((rows // 128, 128), F32), V((cols // 128, 128), F32),
            V((rows // 128, 128), F32), V((cols // 128, 128), F32),
            V((L, ga, rows // 128, 128), F32), V((L, gb, cols // 128, 128), F32),
            V((ga, pad, d), F32), V((L, ga, pad, d), F32),
            V((gb, pad, d), F32), V((L, nz, pad, d), F32), V((L, nz, pad, d), F32),
            *[V(w.shape, F32) for w in weights],
            V((2, 2 * d, weights[3].shape[2]), BF16), V((weights[3].shape[2], 2 * d), BF16),
            dma(8), dma(L), dma(L), dma(L), dma(L, nz), *[dma(L)] * 8, dma(L, cols // 256), dma(L), dma(L),
        ],
        compiler_params=pltpu.CompilerParams(
            collective_id=0, has_side_effects=True, vmem_limit_bytes=48 * 1024 * 1024
        ),
    )(*[pltpu.with_memory_space_constraint(a, pltpu.MemorySpace.HBM) for a in (x, y, *weights)])
    return h[0], h[1]


def solution(mesh):
    size = mesh.shape["row"] * mesh.shape["col"]
    dims = (4, 4, 8) if size == 256 else (2, 2, 2)
    placed = (P(("row", "col"), None), P(("row", "col"), None), P(), P(), P(), P(), P(), P())
    return jax.shard_map(
        functools.partial(align_all, dims),
        mesh=mesh,
        in_specs=placed,
        out_specs=(P(("row", "col"), None), P(("row", "col"), None)),
        check_vma=False,
    )
```
